256 devices in a mesh: rows: 128 (over z, x, y), cols: 2 (over core).
Axes of the slice: x: 4, y: 4, z: 8, core: 2. Of those that a mesh axis runs over, the one named last changes fastest.
Arguments:
- friction: float32 [4096, 8192], P('rows', 'cols'), may hold values from 0.00015625 to 0.015625
- sources: int32 [4096, 8192], P('rows', 'cols'), may hold values from 0 to 1, as said below
Outputs:
- cost: float32 [4096, 8192], P('rows', 'cols')
- overview_one: float32 [2048, 4096], P('rows', 'cols')
- overview_two: float32 [1024, 2048], P('rows', 'cols')
- change: float32 [1], replicated
The draws below stay inside these ranges and needn't reach their ends.
Inputs may be any that keep to these rules, and one draw needn't show every extreme that they name: `sources`: at least one cell of the raster is a source.
All inputs are finite; a program needn't handle non-finite values.
Results may differ from the reference program's by a relative error of at most 0.00002.
Values sent between devices are 32-bit elements; how exact they have to be, the bound alone decides.
A program may use at most 128 MiB of HBM per device.

```python
import math
import jax
import jax.numpy as jnp
from jax import lax

R_DEV = 32
C_DEV = 4096
ITERS = 2
NR = 4096
NC = 8192


def draw_sources(key, part):
    first = jax.random.fold_in(key, 11)
    second = jax.random.fold_in(key, 23)
    third = jax.random.fold_in(key, 37)
    scattered = jax.random.randint(first, (NR, NC), 0, 4 * R_DEV * C_DEV) == 0
    row_pick = jax.random.randint(second, (), 0, NR)
    col_pick = jax.random.randint(third, (), 0, NC)
    forced = (lax.broadcasted_iota(jnp.int32, (NR, NC), 0) == row_pick) & (lax.broadcasted_iota(jnp.int32, (NR, NC), 1) == col_pick)
    return (scattered | forced).astype(jnp.int32)


def levels(rng, extent, cuts, smallest, largest):
    level = 1.0
    for axis_at, blocks in cuts:
        heights = jax.random.uniform(jax.random.fold_in(jax.random.fold_in(rng, 6), axis_at), (blocks,), jnp.float32, smallest / len(cuts), largest / len(cuts))
        level = level * jnp.repeat(jnp.exp(heights), extent[axis_at] // blocks).reshape((-1,) + (1,) * (len(extent) - 1 - axis_at))
    return level


def setup_inputs(seed: int = 0) -> dict:
    keys = jax.random.split(jax.random.key(seed), 3)
    friction = jnp.clip(jnp.exp(math.log(0.015625) - 4.6051702 * jax.random.uniform(keys[0], (NR, NC), jnp.float32) ** levels(keys[0], (NR, NC), ((0, 128), (1, 2)), -0.2, 0.2)), 0.00015625, 0.015625)
    sources = draw_sources(jax.random.fold_in(keys[2], 71), 0)
    return {"friction": friction, "sources": sources}


HUGE = 1e30


def link(earlier, later):
    return (jnp.minimum(later[0], earlier[0] + later[1]), earlier[1] + later[1])


def sweep(field, weights, axis, backward):
    return lax.associative_scan(link, (field, weights), reverse=backward, axis=axis)[0]


def pooled(image):
    height, width = image.shape
    return jnp.min(image.reshape(height // 2, 2, width // 2, 2), axis=(1, 3))


def reference(friction, sources):
    rimmed = jnp.pad(friction, 1)
    centre = rimmed[1:-1, 1:-1]
    w_down = 0.5 * (rimmed[:-2, 1:-1] + centre)
    w_up = 0.5 * (rimmed[2:, 1:-1] + centre)
    w_right = 0.5 * (rimmed[1:-1, :-2] + centre)
    w_left = 0.5 * (rimmed[1:-1, 2:] + centre)
    field = jnp.where(sources == 1, jnp.zeros_like(friction), jnp.full_like(friction, HUGE))
    previous = field
    for step in range(ITERS):
        previous = field
        field = sweep(field, w_down, 0, False)
        field = sweep(field, w_up, 0, True)
        field = sweep(field, w_right, 1, False)
        field = sweep(field, w_left, 1, True)
    change = jnp.max(previous - field).reshape(1)
    overview_one = pooled(field)
    overview_two = pooled(overview_one)
    return field, overview_one, overview_two, change
```

```python
import functools

import jax
import jax.numpy as jnp
from jax import lax
from jax.experimental import pallas as pl
from jax.experimental.pallas import tpu as pltpu
from jax.sharding import PartitionSpec as P

HUGE = 1e30
MESH = pl.DeviceIdType.MESH
ROWS = 32
CHUNKS = 32
LANES = 128
PLANE = 16


def kernel(
    nz, np_, f_hbm, s_hbm, cost_hbm, one_hbm, two_hbm, change_ref,
    fn, sn, h_ref, x_ref, d_ref, u_ref, ht, xt, vf, vb, on, pool, o1, o2,
    s1a, r1a, s2a, r2a, s1b, r1b, s2b, r2b, s3, r3, pre, enter, xs, xr,
    in_sem, out_sem, send1, recv1, send2, recv2, send3, recv3, sendx, recvx,
):
    width = CHUNKS // np_
    row = lax.axis_index("rows")
    core = lax.axis_index("cols")
    z, p = row // np_, row % np_
    tile = (4, 8, LANES)
    part = (width, LANES)

    in_f = pltpu.make_async_copy(f_hbm, fn, in_sem.at[0])
    in_s = pltpu.make_async_copy(s_hbm, sn, in_sem.at[1])
    in_f.start()
    in_s.start()

    def in_plane(k):
        return (z * np_ + (p + k) % np_, core)

    def in_z(k):
        return (((z + k) % nz) * np_ + p, core)

    barrier = pltpu.get_barrier_semaphore()
    for k in range(1, np_):
        pl.semaphore_signal(barrier, inc=1, device_id=in_plane(k), device_id_type=MESH)
    for k in range(1, nz):
        pl.semaphore_signal(barrier, inc=1, device_id=in_z(k), device_id_type=MESH)
    pl.semaphore_signal(barrier, inc=1, device_id=(row, 1 - core), device_id_type=MESH)

    huge = jnp.full(tile, HUGE, jnp.float32)
    zero = jnp.zeros(tile, jnp.float32)

    in_f.wait()
    in_s.wait()

    def spread(b, _):
        for s in range(8):
            for g in range(4):
                lines = pl.ds((b * 32 + g * 8) * 8 + s, 8, stride=8)
                h_ref[b * 8 + s, g] = 0.5 * fn[lines, :]
                x_ref[b * 8 + s, g] = jnp.where(sn[lines, :] == 1, 0.0, HUGE)
        return 0

    lax.fori_loop(0, ROWS // 8, spread, 0)

    def first_local(b, carry):
        down, up, hd, hu, total = carry
        for s in range(8):
            i = b * 8 + s
            h = h_ref[i]
            down = jnp.minimum(x_ref[i], down + (hd + h))
            total = total + h
            hd = h
            h = h_ref[ROWS - 1 - i]
            up = jnp.minimum(x_ref[ROWS - 1 - i], up + (hu + h))
            hu = h
        return (down, up, hd, hu, total)

    def second_local(b, carry):
        down, up, hd, hu, far_d, far_u, most = carry
        for s in range(8):
            i = b * 8 + s
            h, x = h_ref[i], x_ref[i]
            down = jnp.minimum(x, down + (hd + h))
            far_d = jnp.maximum(x, far_d - (hd + h))
            most = jnp.maximum(most, x - down)
            hd = h
            h, x = h_ref[ROWS - 1 - i], x_ref[ROWS - 1 - i]
            up = jnp.minimum(x, up + (hu + h))
            far_u = jnp.maximum(x, far_u - (hu + h))
            most = jnp.maximum(most, x - up)
            hu = h
        return (down, up, hd, hu, far_d, far_u, most)

    def put(to, item, value):
        for q in range(np_):
            line = q * width
            to[q, item] = value[line // 8, line % 8 : line % 8 + width, :]

    def exchange(to, got, peer, count, mine, sends, recvs):
        copies = []
        for k in range(1, count):
            target = (mine + k) % count
            copy = pltpu.make_async_remote_copy(
                src_ref=to.at[target],
                dst_ref=got.at[mine],
                send_sem=sends.at[k],
                recv_sem=recvs.at[k],
                device_id=peer(k),
                device_id_type=MESH,
            )
            copy.start()
            copies.append(copy)
        return copies

    def finish(copies):
        for copy in copies:
            copy.wait()

    my_z = jnp.full(part, z, jnp.int32)

    def pick(k, new, old):
        return jnp.where(my_z == k, new, old)

    def vertical(step):
        s1, r1, s2, r2 = ((s1a, r1a, s2a, r2a), (s1b, r1b, s2b, r2b))[step]
        if step == 0:
            down, up, hd, hu, total = lax.fori_loop(
                0, ROWS // 8, first_local, (huge, huge, zero, zero, zero)
            )
            values = (up + hu, down + hd, 2.0 * total)
        else:
            down, up, hd, hu, far_d, far_u, most = lax.fori_loop(
                0, ROWS // 8, second_local, (huge, huge, zero, zero, -huge, -huge, zero)
            )
            values = (up + hu, down + hd, far_u - hu, far_d - hd, most)
        items = len(values)
        for item, value in enumerate(values):
            put(s1, item, value)
        if step == 0:
            pl.semaphore_wait(barrier, np_ + nz - 1)
        copies = exchange(s1, r1, in_plane, np_, p, send1.at[step], recv1.at[step])
        for item in range(items):
            r1[p, item] = s1[p, item]
        finish(copies)

        near = jnp.full(part, HUGE, jnp.float32)
        none = jnp.zeros(part, jnp.float32)
        b, a, s_down, s_up, far_d, far_u, most = near, near, none, none, -near, -near, none
        for q in range(np_):
            r_a, r_b = r1[q, 0], r1[q, 1]
            if step == 0:
                s = r1[q, 2]
                pre[q, 2] = s_down
                s_down = s_down + s
            else:
                s = r1a[q, 2]
                most = jnp.maximum(most, jnp.maximum(far_d - r_a, r1[q, 2] - b))
                most = jnp.maximum(most, r1[q, 4])
                far_d = jnp.maximum(r1[q, 3], far_d - s)
            pre[q, 0] = b
            b = jnp.minimum(r_b, b + s)
        for q in range(np_ - 1, -1, -1):
            s = r1a[q, 2]
            if step == 0:
                pre[q, 3] = s_up
                s_up = s_up + s
            else:
                far_u = jnp.maximum(r1[q, 2], far_u - s)
            pre[q, 1] = a
            a = jnp.minimum(r1[q, 0], a + s)
        values = (a, b, s_down) if step == 0 else (a, b, far_u, far_d, most)
        for k in range(nz):
            for item, value in enumerate(values):
                s2[k, item] = value
        copies = exchange(s2, r2, in_z, nz, z, send2.at[step], recv2.at[step])
        for item in range(items):
            r2[z, item] = values[item]
        finish(copies)

        b, a, far_d, most = near, near, -near, none
        in_d, in_u = near, near
        for k in range(nz):
            in_d = pick(k, b, in_d)
            s = r2a[k, 2]
            if step == 1:
                most = jnp.maximum(most, jnp.maximum(far_d - r2[k, 0], r2[k, 2] - b))
                most = jnp.maximum(most, r2[k, 4])
                far_d = jnp.maximum(r2[k, 3], far_d - s)
            b = jnp.minimum(r2[k, 1], b + s)
        for k in range(nz - 1, -1, -1):
            in_u = pick(k, a, in_u)
            a = jnp.minimum(r2[k, 0], a + r2a[k, 2])
        to, got = s3.at[step], r3.at[step]
        for q in range(np_):
            to[q, 0] = jnp.minimum(pre[q, 0], in_d + pre[q, 2])
            to[q, 1] = jnp.minimum(pre[q, 1], in_u + pre[q, 3])
            to[q, 2] = most
        copies = exchange(to, got, in_plane, np_, p, send3.at[step], recv3.at[step])
        for item in range(3):
            got[p, item] = to[p, item]
        finish(copies)
        most = got[0, 2]
        for q in range(np_):
            line = q * width
            for item in range(2):
                enter[item, line // 8, line % 8 : line % 8 + width, :] = got[q, item]
            most = jnp.maximum(most, got[q, 2])

        def final(b, carry):
            down, up, hd, hu = carry
            for s in range(8):
                i = b * 8 + s
                h = h_ref[i]
                down = jnp.minimum(x_ref[i], down + (hd + h))
                d_ref[i] = down
                hd = h
                h = h_ref[ROWS - 1 - i]
                up = jnp.minimum(x_ref[ROWS - 1 - i], up + (hu + h))
                u_ref[ROWS - 1 - i] = up
                hu = h
            return (down, up, hd, hu)

        lax.fori_loop(0, ROWS // 8, final, (enter[0], enter[1], zero, zero))
        return most

    lane = lax.broadcasted_iota(jnp.int32, (8, LANES), 1)
    sub = lax.broadcasted_iota(jnp.int32, (8, LANES), 0)
    inner, outer = lane % 8, sub % 4
    huge2 = jnp.full((8, LANES), HUGE, jnp.float32)
    zero2 = jnp.zeros((8, LANES), jnp.float32)

    def block(load, j):
        return load(pl.ds((j // 4) * 16, 16), j % 4).reshape(LANES, LANES)

    def scan_all(c, s, axis, size, place, forward):
        step = 1 if forward else -1
        extent = c.shape[axis]
        at = place if forward else size - 1 - place
        run, length = huge2, zero2
        for k in range(size - 1, 0, -1):
            ck = pltpu.roll(c, (step * k) % extent, axis)
            sk = pltpu.roll(s, (step * k) % extent, axis)
            here = at >= k
            run = jnp.where(here, jnp.minimum(ck, run + sk), run)
            length = jnp.where(here, length + sk, length)
        before, passed = run, length
        run, length = jnp.minimum(c, run + s), length + s
        for k in range(1, size):
            ck = pltpu.roll(c, (-step * k) % extent, axis)
            sk = pltpu.roll(s, (-step * k) % extent, axis)
            here = at + k < size
            run = jnp.where(here, jnp.minimum(ck, run + sk), run)
            length = jnp.where(here, length + sk, length)
        return before, passed, run, length

    def horizontal(step, most):
        for j in range(8):
            rows = pl.ds(j, LANES, stride=8)
            xt[rows, :] = block(lambda r, g: jnp.minimum(d_ref[r, g], u_ref[r, g]), j).T
            if step == 0:
                ht[rows, :] = block(lambda r, g: h_ref[r, g], j).T

        def at(i):
            return pl.ds(pl.multiple_of(i * 8, 8), 8)

        def local(b, carry):
            right, left, hr, hl, total = carry
            for s in range(8):
                i = b * 8 + s
                h = ht[at(i), :]
                right = jnp.minimum(xt[at(i), :], right + (hr + h))
                total = total + h
                hr = h
                h = ht[at(LANES - 1 - i), :]
                left = jnp.minimum(xt[at(LANES - 1 - i), :], left + (hl + h))
                hl = h
            return (right, left, hr, hl, total)

        right, left, hr, hl, total = lax.fori_loop(
            0, LANES // 8, local, (huge2, huge2, zero2, zero2, zero2)
        )
        total = 2.0 * total
        right, left = right + hr, left + hl
        fc, fs, f_all, fs_all = scan_all(right, total, 1, 8, inner, True)
        bc, bs, b_all, bs_all = scan_all(left, total, 1, 8, inner, False)
        gfc, gfs, gf_all, _ = scan_all(f_all, fs_all, 0, 4, outer, True)
        gbc, gbs, gb_all, _ = scan_all(b_all, bs_all, 0, 4, outer, False)
        first = jnp.full((8, LANES), core, jnp.int32) == 0
        xs[step, 0] = jnp.where(first, gf_all, gb_all)
        xs[step, 1] = jnp.broadcast_to(jnp.max(most, axis=0, keepdims=True), (8, LANES))
        copy = pltpu.make_async_remote_copy(
            src_ref=xs.at[step],
            dst_ref=xr.at[step],
            send_sem=sendx.at[step],
            recv_sem=recvx.at[step],
            device_id=(row, 1 - core),
            device_id_type=MESH,
        )
        copy.start()
        copy.wait()
        other = xr[step, 0]
        in_f = jnp.where(first, HUGE, other)
        in_b = jnp.where(first, other, HUGE)
        in_f = jnp.minimum(fc, jnp.minimum(gfc, in_f + gfs) + fs)
        in_b = jnp.minimum(bc, jnp.minimum(gbc, in_b + gbs) + bs)

        def final(b, carry):
            right, left, hr, hl = carry
            for s in range(8):
                i = b * 8 + s
                h = ht[at(i), :]
                right = jnp.minimum(xt[at(i), :], right + (hr + h))
                vf[at(i), :] = right
                hr = h
                h = ht[at(LANES - 1 - i), :]
                left = jnp.minimum(xt[at(LANES - 1 - i), :], left + (hl + h))
                vb[at(LANES - 1 - i), :] = left
                hl = h
            return (right, left, hr, hl)

        lax.fori_loop(0, LANES // 8, final, (in_f, in_b, zero2, zero2))

    most = vertical(0)
    horizontal(0, most)
    for j in range(8):
        rows = pl.ds(j, LANES, stride=8)
        back = jnp.minimum(vf[rows, :], vb[rows, :]).T
        x_ref[pl.ds((j // 4) * 16, 16), j % 4] = back.reshape(16, 8, LANES)
    most = vertical(1)
    horizontal(1, most)

    def merge(b, _):
        lines = pl.ds(pl.multiple_of(b * LANES, LANES), LANES)
        xt[lines, :] = jnp.minimum(vf[lines, :], vb[lines, :])
        return 0

    lax.fori_loop(0, 8, merge, 0)
    for j in range(8):
        back = xt[pl.ds(j, LANES, stride=8), :].T
        for r in range(16):
            i = (j // 4) * 16 + r
            lines = pl.ds(((i // 8) * 32 + (j % 4) * 8) * 8 + i % 8, 8, stride=8)
            on[lines, :] = back[r * 8 : (r + 1) * 8, :]
    out_cost = pltpu.make_async_copy(on, cost_hbm, out_sem.at[0])
    out_cost.start()

    for j in range(8):
        pair = jnp.minimum(xt[pl.ds(j, 64, stride=16), :], xt[pl.ds(j + 8, 64, stride=16), :])
        lines = jnp.concatenate([pair, pair], axis=0).T.reshape(8, 2, 8, LANES)
        pool[pl.ds((j // 4) * 8, 8), j % 4] = jnp.minimum(lines[:, 0], lines[:, 1])
        ht[pl.ds(j, 64, stride=8), :] = pair
    for a in range(16):
        for g in range(2):
            halves = [
                jnp.concatenate([pool[a, 2 * g + t, pl.ds(i, 4, stride=2), :] for t in range(2)], axis=0)
                for i in range(2)
            ]
            lines = pl.ds(((a // 8) * 16 + g * 8) * 8 + a % 8, 8, stride=8)
            o1[lines, :] = jnp.where(lane < 64, halves[0], halves[1])
    out_one = pltpu.make_async_copy(o1, one_hbm, out_sem.at[1])
    out_one.start()

    for j in range(8):
        quad = jnp.minimum(ht[pl.ds(j, 32, stride=16), :], ht[pl.ds(j + 8, 32, stride=16), :])
        lines = jnp.concatenate([quad] * 4, axis=0).T.reshape(4, 4, 8, LANES)
        lines = jnp.minimum(
            jnp.minimum(lines[:, 0], lines[:, 1]), jnp.minimum(lines[:, 2], lines[:, 3])
        )
        pool[pl.ds(16 + (j // 4) * 4, 4), j % 4] = lines
    for a in range(8):
        quarters = [
            jnp.concatenate([pool[16 + a, g, pl.ds(i, 2, stride=4), :] for g in range(4)], axis=0)
            for i in range(4)
        ]
        low = jnp.where(lane < 32, quarters[0], quarters[1])
        high = jnp.where(lane < 96, quarters[2], quarters[3])
        o2[pl.ds(a, 8, stride=8), :] = jnp.where(lane < 64, low, high)
    out_two = pltpu.make_async_copy(o2, two_hbm, out_sem.at[2])
    out_two.start()

    change_ref[0] = jnp.max(jnp.maximum(xs[1, 1], xr[1, 1]))
    out_cost.wait()
    out_one.wait()
    out_two.wait()


def lines_of(block):
    height, length = block.shape
    return (
        block.reshape(height // 8, 8, length // LANES, LANES)
        .transpose(0, 2, 1, 3)
        .reshape(-1, LANES)
    )


def block_of(lines, height):
    return (
        lines.reshape(height // 8, -1, 8, LANES).transpose(0, 2, 1, 3).reshape(height, -1)
    )


def shards(nz, np_, friction, sources):
    width = CHUNKS // np_
    f32 = jnp.float32
    anywhere = pl.BlockSpec(memory_space=pl.ANY)
    field = pltpu.VMEM((ROWS, 4, 8, LANES), f32)
    flat = pltpu.VMEM((ROWS * CHUNKS, LANES), f32)
    dma = pltpu.SemaphoreType.DMA
    cost, one, two, change = pl.pallas_call(
        functools.partial(kernel, nz, np_),
        out_shape=(
            jax.ShapeDtypeStruct((1024, LANES), f32),
            jax.ShapeDtypeStruct((256, LANES), f32),
            jax.ShapeDtypeStruct((64, LANES), f32),
            jax.ShapeDtypeStruct((1,), f32),
        ),
        in_specs=[anywhere, anywhere],
        out_specs=(anywhere, anywhere, anywhere, pl.BlockSpec(memory_space=pltpu.SMEM)),
        scratch_shapes=[
            flat,
            pltpu.VMEM((ROWS * CHUNKS, LANES), jnp.int32),
            field, field, field, field,
            flat, flat, flat, flat,
            flat,
            pltpu.VMEM((24, 4, 8, LANES), f32),
            pltpu.VMEM((256, LANES), f32),
            pltpu.VMEM((64, LANES), f32),
            pltpu.VMEM((np_, 3, width, LANES), f32),
            pltpu.VMEM((np_, 3, width, LANES), f32),
            pltpu.VMEM((nz, 3, width, LANES), f32),
            pltpu.VMEM((nz, 3, width, LANES), f32),
            pltpu.VMEM((np_, 5, width, LANES), f32),
            pltpu.VMEM((np_, 5, width, LANES), f32),
            pltpu.VMEM((nz, 5, width, LANES), f32),
            pltpu.VMEM((nz, 5, width, LANES), f32),
            pltpu.VMEM((2, np_, 3, width, LANES), f32),
            pltpu.VMEM((2, np_, 3, width, LANES), f32),
            pltpu.VMEM((np_, 4, width, LANES), f32),
            pltpu.VMEM((2, 4, 8, LANES), f32),
            pltpu.VMEM((2, 2, 8, LANES), f32),
            pltpu.VMEM((2, 2, 8, LANES), f32),
            dma((2,)),
            dma((3,)),
            dma((2, np_)), dma((2, np_)),
            dma((2, nz)), dma((2, nz)),
            dma((2, np_)), dma((2, np_)),
            dma((2,)), dma((2,)),
        ],
        compiler_params=pltpu.CompilerParams(collective_id=0, has_side_effects=True),
    )(lines_of(friction), lines_of(sources))
    return (block_of(cost, 32), block_of(one, 16), block_of(two, 8), change)


def solution(mesh):
    slabs = mesh.shape["rows"]
    plane = min(PLANE, slabs // 2)
    return jax.shard_map(
        functools.partial(shards, slabs // plane, plane),
        mesh=mesh,
        in_specs=(P("rows", "cols"), P("rows", "cols")),
        out_specs=(P("rows", "cols"), P("rows", "cols"), P("rows", "cols"), P()),
        check_vma=False,
    )
```

```python
import functools

import jax
import jax.numpy as jnp
from jax import lax
from jax.experimental import pallas as pl
from jax.experimental.pallas import tpu as pltpu
from jax.sharding import PartitionSpec as P

HUGE = 1e30
MESH = pl.DeviceIdType.MESH
ROWS = 32
CHUNKS = 32
LANES = 128
PLANE = (4, 4)
HUB = 1
PARTS = 4
STEPS = LANES // PARTS


def far_first(sizes):
    offsets = [()]
    for size in sizes:
        offsets = [(*o, k) for o in offsets for k in range(size)]
    hops = lambda o: sum(min(k, s - k) for k, s in zip(o, sizes))
    return sorted((o for o in offsets if any(o)), key=hops, reverse=True)


def kernel(
    nz, plane, f_hbm, s_hbm, lines_ref, change_ref,
    fn, sn, h_ref, x_ref, d_ref, u_ref, ht, xt, vf, vb,
    s1a, r1a, s2a, r2a, s1b, r1b, s2b, r2b, s3, r3, pre, enter, xs, xr, paths,
    in_sem, send1, recv1, send2, recv2, send3, recv3, sendx, recvx,
):
    px, py = plane
    np_ = px * py
    width = CHUNKS // np_
    row = lax.axis_index("rows")
    core = lax.axis_index("cols")
    z, p = row // np_, row % np_
    x, y = p // py, p % py
    other_core = 1 - core
    hub = core == HUB
    tile = (4, 8, LANES)
    part = (2, width, LANES)
    near_plane = far_first(plane)
    near_z = far_first((nz,))

    def in_copies(b):
        lines = pl.ds(pl.multiple_of(b * 256, 256), 256)
        return (
            pltpu.make_async_copy(f_hbm.at[lines], fn.at[lines], in_sem.at[0, b]),
            pltpu.make_async_copy(s_hbm.at[lines], sn.at[lines], in_sem.at[1, b]),
        )

    for b in range(4):
        for copy in in_copies(b):
            copy.start()

    def slot(k):
        dx, dy = near_plane[k]
        return ((x + dx) % px) * py + (y + dy) % py

    def z_slot(k):
        return (z + near_z[k][0]) % nz

    barrier = pltpu.get_barrier_semaphore()

    def greet(device):
        pl.semaphore_signal(barrier, inc=1, device_id=device, device_id_type=MESH)

    for k in range(np_ - 1):
        greet((z * np_ + slot(k), HUB))

    @pl.when(hub)
    def _():
        for k in range(np_ - 1):
            greet((z * np_ + slot(k), 1 - HUB))
        for k in range(nz - 1):
            greet((z_slot(k) * np_ + p, HUB))

    greet((row, other_core))

    def wait_for_peers():
        @pl.when(hub)
        def _():
            pl.semaphore_wait(barrier, 2 * (np_ - 1) + nz)

        @pl.when(jnp.logical_not(hub))
        def _():
            pl.semaphore_wait(barrier, np_)

    huge = jnp.full(tile, HUGE, jnp.float32)
    zero = jnp.zeros(tile, jnp.float32)

    def spread(b, _):
        for copy in in_copies(b):
            copy.wait()
        for s in range(8):
            for g in range(4):
                lines = pl.ds((b * 32 + g * 8) * 8 + s, 8, stride=8)
                h_ref[b * 8 + s, g] = 0.5 * fn[lines, :]
                x_ref[b * 8 + s, g] = jnp.where(sn[lines, :] == 1, 0.0, HUGE)
        return 0

    lax.fori_loop(0, ROWS // 8, spread, 0)

    def first_local(b, carry):
        down, up, hd, hu, total = carry
        for s in range(8):
            i = b * 8 + s
            h = h_ref[i]
            down = jnp.minimum(x_ref[i], down + (hd + h))
            total = total + h
            hd = h
            h = h_ref[ROWS - 1 - i]
            up = jnp.minimum(x_ref[ROWS - 1 - i], up + (hu + h))
            hu = h
        return (down, up, hd, hu, total)

    def second_local(b, carry):
        down, up, hd, hu, far_d, far_u, most = carry
        for s in range(8):
            i = b * 8 + s
            h, v = h_ref[i], x_ref[i]
            down = jnp.minimum(v, down + (hd + h))
            far_d = jnp.maximum(v, far_d - (hd + h))
            most = jnp.maximum(most, v - down)
            hd = h
            h, v = h_ref[ROWS - 1 - i], x_ref[ROWS - 1 - i]
            up = jnp.minimum(v, up + (hu + h))
            far_u = jnp.maximum(v, far_u - (hu + h))
            most = jnp.maximum(most, v - up)
            hu = h
        return (down, up, hd, hu, far_d, far_u, most)

    def put(to, item, value):
        for q in range(np_):
            line = q * width
            to[q, item] = value[line // 8, line % 8 : line % 8 + width, :]

    def remote(src, dst, send, recv, device):
        return pltpu.make_async_remote_copy(
            src_ref=src, dst_ref=dst, send_sem=send, recv_sem=recv,
            device_id=device, device_id_type=MESH,
        )

    my_z = jnp.full(part, z, jnp.int32)

    def pick(k, new, old):
        return jnp.where(my_z == k, new, old)

    def vertical(step, window):
        s1, r1, s2, r2 = ((s1a, r1a, s2a, r2a), (s1b, r1b, s2b, r2b))[step]
        if step == 0:
            down, up, hd, hu, total = lax.fori_loop(
                0, ROWS // 8, first_local, (huge, huge, zero, zero, zero)
            )
            values = (up + hu, down + hd, 2.0 * total)
        else:
            down, up, hd, hu, far_d, far_u, most = lax.fori_loop(
                0, ROWS // 8, second_local, (huge, huge, zero, zero, -huge, -huge, zero)
            )
            values = (up + hu, down + hd, far_u - hu, far_d - hd, most)
        items = len(values)
        for item, value in enumerate(values):
            put(s1, item, value)
        if step == 0:
            wait_for_peers()
        copies = []
        for k in range(np_ - 1):
            copy = remote(
                s1.at[slot(k)], r1.at[p, :, core], send1.at[step, k], recv1.at[step, core, k],
                (z * np_ + slot(k), HUB),
            )
            copy.start()
            copies.append(copy)
        last = np_ - 1
        to_hub = remote(
            s1.at[p], r1.at[p, :, core], send1.at[step, last], recv1.at[step, core, last], (row, HUB)
        )

        @pl.when(jnp.logical_not(hub))
        def _():
            to_hub.start()

        window()

        for copy in copies:
            copy.wait_send()

        @pl.when(jnp.logical_not(hub))
        def _():
            to_hub.wait_send()

        to, got = s3.at[step], r3.at[step]

        @pl.when(hub)
        def _():
            for item in range(items):
                r1[p, item, HUB] = s1[p, item]
            for k in range(np_):
                for half in range(2):
                    if k == last and half == HUB:
                        continue
                    remote(
                        s1.at[p], r1.at[p, :, half], send1.at[step, k], recv1.at[step, half, k], (row, HUB)
                    ).wait_recv()
            near = jnp.full(part, HUGE, jnp.float32)
            none = jnp.zeros(part, jnp.float32)
            b, a, s_down, s_up, far_d, far_u, most = near, near, none, none, -near, -near, none
            for q in range(np_):
                r_a, r_b = r1[q, 0], r1[q, 1]
                if step == 0:
                    s = r1[q, 2]
                    pre[q, 2] = s_down
                    s_down = s_down + s
                else:
                    s = r1a[q, 2]
                    most = jnp.maximum(most, jnp.maximum(far_d - r_a, r1[q, 2] - b))
                    most = jnp.maximum(most, r1[q, 4])
                    far_d = jnp.maximum(r1[q, 3], far_d - s)
                pre[q, 0] = b
                b = jnp.minimum(r_b, b + s)
            for q in range(np_ - 1, -1, -1):
                s = r1a[q, 2]
                if step == 0:
                    pre[q, 3] = s_up
                    s_up = s_up + s
                else:
                    far_u = jnp.maximum(r1[q, 2], far_u - s)
                pre[q, 1] = a
                a = jnp.minimum(r1[q, 0], a + s)
            values = (a, b, s_down) if step == 0 else (a, b, far_u, far_d, most)
            for item, value in enumerate(values):
                s2[item] = value
            copies = []
            for k in range(nz - 1):
                copy = remote(
                    s2, r2.at[z], send2.at[step, k], recv2.at[step, k], (z_slot(k) * np_ + p, HUB)
                )
                copy.start()
                copies.append(copy)
            for item in range(items):
                r2[z, item] = values[item]
            for copy in copies:
                copy.wait()

            b, a, far_d, most = near, near, -near, none
            in_d, in_u = near, near
            for k in range(nz):
                in_d = pick(k, b, in_d)
                s = r2a[k, 2]
                if step == 1:
                    most = jnp.maximum(most, jnp.maximum(far_d - r2[k, 0], r2[k, 2] - b))
                    most = jnp.maximum(most, r2[k, 4])
                    far_d = jnp.maximum(r2[k, 3], far_d - s)
                b = jnp.minimum(r2[k, 1], b + s)
            for k in range(nz - 1, -1, -1):
                in_u = pick(k, a, in_u)
                a = jnp.minimum(r2[k, 0], a + r2a[k, 2])
            most = jnp.maximum(most[0], most[1])
            for q in range(np_):
                to[q, 0] = jnp.minimum(pre[q, 0], in_d + pre[q, 2])
                to[q, 1] = jnp.minimum(pre[q, 1], in_u + pre[q, 3])
                to[q, 2, 0] = most
                to[q, 2, 1] = most
            copies = []
            for k in range(np_):
                for half in range(2):
                    if k == last and half == HUB:
                        continue
                    q = p if k == last else slot(k)
                    copy = remote(
                        to.at[q, :, half], got.at[p], send3.at[step, half, k], recv3.at[step, k],
                        (z * np_ + q, half),
                    )
                    copy.start()
                    copies.append(copy)
            for item in range(3):
                got[p, item] = to[p, item, HUB]
            for copy in copies:
                copy.wait_send()

        def from_hub(k):
            return remote(
                to.at[p, :, 0], got.at[p], send3.at[step, 0, k], recv3.at[step, k], (row, HUB)
            )

        for k in range(last):
            from_hub(k).wait_recv()

        @pl.when(jnp.logical_not(hub))
        def _():
            from_hub(last).wait_recv()

        most = got[0, 2]
        for q in range(np_):
            line = q * width
            for item in range(2):
                enter[item, line // 8, line % 8 : line % 8 + width, :] = got[q, item]
            most = jnp.maximum(most, got[q, 2])

        def final(b, carry):
            down, up, hd, hu = carry
            for s in range(8):
                i = b * 8 + s
                h = h_ref[i]
                down = jnp.minimum(x_ref[i], down + (hd + h))
                d_ref[i] = down
                hd = h
                h = h_ref[ROWS - 1 - i]
                up = jnp.minimum(x_ref[ROWS - 1 - i], up + (hu + h))
                u_ref[ROWS - 1 - i] = up
                hu = h
            return (down, up, hd, hu)

        lax.fori_loop(0, ROWS // 8, final, (enter[0], enter[1], zero, zero))
        return most

    lane = lax.broadcasted_iota(jnp.int32, (8, LANES), 1)
    sub = lax.broadcasted_iota(jnp.int32, (8, LANES), 0)
    inner, outer = lane % 8, sub % 4
    huge2 = jnp.full((8, LANES), HUGE, jnp.float32)
    zero2 = jnp.zeros((8, LANES), jnp.float32)

    def block(load, j):
        return load(pl.ds((j // 4) * 16, 16), j % 4).reshape(LANES, LANES)

    def at(i):
        return pl.ds(pl.multiple_of(i * 8, 8), 8)

    def chunk_path(shift):
        return paths[11 + shift]

    def group_path(shift):
        return paths[22 + shift]

    def measure():
        for j in range(8):
            ht[pl.ds(j, LANES, stride=8), :] = block(lambda r, g: h_ref[r, g], j).T

        def add(b, sums):
            return tuple(
                sum((ht[at(k * STEPS + b * 8 + s), :] for s in range(8)), start=sums[k])
                for k in range(PARTS)
            )

        sums = lax.fori_loop(0, STEPS // 8, add, (zero2,) * PARTS)
        for k in range(PARTS):
            paths[k] = 2.0 * sums[k]
        whole = 2.0 * (sums[0] + sums[1] + sums[2] + sums[3])
        before = after = zero2
        for k in range(-7, 8):
            rolled = pltpu.roll(whole, k % LANES, 1)
            paths[11 + k] = rolled
            if k > 0:
                before = jnp.where(inner >= k, before + rolled, before)
            if k < 0:
                after = jnp.where(inner - k < 8, after + rolled, after)
        paths[26] = before
        paths[27] = after
        whole = before + whole + after
        before = after = zero2
        for k in range(-3, 4):
            rolled = pltpu.roll(whole, k % 8, 0)
            paths[22 + k] = rolled
            if k > 0:
                before = jnp.where(outer >= k, before + rolled, before)
            if k < 0:
                after = jnp.where(outer - k < 4, after + rolled, after)
        paths[28] = before
        paths[29] = after

    def scan_all(c, path, axis, size, place, forward):
        step = 1 if forward else -1
        extent = c.shape[axis]
        at_place = place if forward else size - 1 - place
        run = huge2
        for k in range(size - 1, 0, -1):
            ck = pltpu.roll(c, (step * k) % extent, axis)
            run = jnp.where(at_place >= k, jnp.minimum(ck, run + path(step * k)), run)
        before = run
        run = jnp.minimum(c, run + path(0))
        for k in range(1, size):
            ck = pltpu.roll(c, (-step * k) % extent, axis)
            run = jnp.where(at_place + k < size, jnp.minimum(ck, run + path(-step * k)), run)
        return before, run

    def horizontal(step):
        for j in range(8):
            rows = pl.ds(j, LANES, stride=8)
            xt[rows, :] = block(lambda r, g: jnp.minimum(d_ref[r, g], u_ref[r, g]), j).T

        def sweep(start_f, start_b, store):
            def some(b, carry):
                right, left, hr, hl = (list(c) for c in carry)
                for s in range(8):
                    for k in range(PARTS):
                        i = k * STEPS + b * 8 + s
                        h = ht[at(i), :]
                        right[k] = jnp.minimum(xt[at(i), :], right[k] + (hr[k] + h))
                        if store:
                            vf[at(i), :] = right[k]
                        hr[k] = h
                        i = (k + 1) * STEPS - 1 - (b * 8 + s)
                        h = ht[at(i), :]
                        left[k] = jnp.minimum(xt[at(i), :], left[k] + (hl[k] + h))
                        if store:
                            vb[at(i), :] = left[k]
                        hl[k] = h
                return (tuple(right), tuple(left), tuple(hr), tuple(hl))

            zeros = (zero2,) * PARTS
            return lax.fori_loop(0, STEPS // 8, some, (start_f, start_b, zeros, zeros))

        right, left, hr, hl = sweep((huge2,) * PARTS, (huge2,) * PARTS, False)
        right = [r + h for r, h in zip(right, hr)]
        left = [r + h for r, h in zip(left, hl)]
        c_f, c_b = right[0], left[-1]
        for k in range(1, PARTS):
            c_f = jnp.minimum(right[k], c_f + paths[k])
            c_b = jnp.minimum(left[-1 - k], c_b + paths[PARTS - 1 - k])
        fc, f_all = scan_all(c_f, chunk_path, 1, 8, inner, True)
        bc, b_all = scan_all(c_b, chunk_path, 1, 8, inner, False)
        gfc, gf_all = scan_all(f_all, group_path, 0, 4, outer, True)
        gbc, gb_all = scan_all(b_all, group_path, 0, 4, outer, False)
        first = jnp.full((8, LANES), core, jnp.int32) == 0
        xs[step] = jnp.where(first, gf_all, gb_all)
        copy = remote(xs.at[step], xr.at[step], sendx.at[step], recvx.at[step], (row, other_core))
        copy.start()
        copy.wait()
        other = xr[step]
        in_f = jnp.where(first, HUGE, other)
        in_b = jnp.where(first, other, HUGE)
        in_f = [jnp.minimum(fc, jnp.minimum(gfc, in_f + paths[28]) + paths[26])]
        in_b = [jnp.minimum(bc, jnp.minimum(gbc, in_b + paths[29]) + paths[27])]
        for k in range(PARTS - 1):
            in_f.append(jnp.minimum(right[k], in_f[k] + paths[k]))
            in_b.append(jnp.minimum(left[-1 - k], in_b[k] + paths[PARTS - 1 - k]))
        sweep(tuple(in_f), tuple(in_b[::-1]), True)

    vertical(0, measure)
    horizontal(0)
    for j in range(8):
        rows = pl.ds(j, LANES, stride=8)
        back = jnp.minimum(vf[rows, :], vb[rows, :]).T
        x_ref[pl.ds((j // 4) * 16, 16), j % 4] = back.reshape(16, 8, LANES)
    most = vertical(1, lambda: None)
    horizontal(1)
    change_ref[0] = jnp.max(most)

    def merge(b, _):
        lines = pl.ds(pl.multiple_of(b * LANES, LANES), LANES)
        lines_ref[lines, :] = jnp.minimum(vf[lines, :], vb[lines, :])
        return 0

    lax.fori_loop(0, 8, merge, 0)


def finish(xt, most, cost_hbm, one_hbm, two_hbm, change_ref, on, pairs, pool, o1, o2, out_sem):
    lane = lax.broadcasted_iota(jnp.int32, (8, LANES), 1)
    for j in range(8):
        back = xt[pl.ds(j, LANES, stride=8), :].T
        for r in range(16):
            i = (j // 4) * 16 + r
            lines = pl.ds(((i // 8) * 32 + (j % 4) * 8) * 8 + i % 8, 8, stride=8)
            on[lines, :] = back[r * 8 : (r + 1) * 8, :]
    out_cost = pltpu.make_async_copy(on, cost_hbm, out_sem.at[0])
    out_cost.start()

    for j in range(8):
        pair = jnp.minimum(xt[pl.ds(j, 64, stride=16), :], xt[pl.ds(j + 8, 64, stride=16), :])
        lines = jnp.concatenate([pair, pair], axis=0).T.reshape(8, 2, 8, LANES)
        pool[pl.ds((j // 4) * 8, 8), j % 4] = jnp.minimum(lines[:, 0], lines[:, 1])
        pairs[pl.ds(j, 64, stride=8), :] = pair
    for a in range(16):
        for g in range(2):
            halves = [
                jnp.concatenate([pool[a, 2 * g + t, pl.ds(i, 4, stride=2), :] for t in range(2)], axis=0)
                for i in range(2)
            ]
            lines = pl.ds(((a // 8) * 16 + g * 8) * 8 + a % 8, 8, stride=8)
            o1[lines, :] = jnp.where(lane < 64, halves[0], halves[1])
    out_one = pltpu.make_async_copy(o1, one_hbm, out_sem.at[1])
    out_one.start()

    for j in range(8):
        quad = jnp.minimum(pairs[pl.ds(j, 32, stride=16), :], pairs[pl.ds(j + 8, 32, stride=16), :])
        lines = jnp.concatenate([quad] * 4, axis=0).T.reshape(4, 4, 8, LANES)
        lines = jnp.minimum(
            jnp.minimum(lines[:, 0], lines[:, 1]), jnp.minimum(lines[:, 2], lines[:, 3])
        )
        pool[pl.ds(16 + (j // 4) * 4, 4), j % 4] = lines
    for a in range(8):
        quarters = [
            jnp.concatenate([pool[16 + a, g, pl.ds(i, 2, stride=4), :] for g in range(4)], axis=0)
            for i in range(4)
        ]
        low = jnp.where(lane < 32, quarters[0], quarters[1])
        high = jnp.where(lane < 96, quarters[2], quarters[3])
        o2[pl.ds(a, 8, stride=8), :] = jnp.where(lane < 64, low, high)
    out_two = pltpu.make_async_copy(o2, two_hbm, out_sem.at[2])
    out_two.start()
    change_ref[0] = most[0]
    out_cost.wait()
    out_one.wait()
    out_two.wait()


def lines_of(block):
    height, length = block.shape
    return (
        block.reshape(height // 8, 8, length // LANES, LANES)
        .transpose(0, 2, 1, 3)
        .reshape(-1, LANES)
    )


def block_of(lines, height):
    return lines.reshape(height // 8, -1, 8, LANES).transpose(0, 2, 1, 3).reshape(height, -1)


def shards(nz, plane, friction, sources):
    np_ = plane[0] * plane[1]
    width = CHUNKS // np_
    f32 = jnp.float32
    anywhere = pl.BlockSpec(memory_space=pltpu.HBM)
    in_vmem = pl.BlockSpec(memory_space=pltpu.VMEM)
    in_smem = pl.BlockSpec(memory_space=pltpu.SMEM)
    field = pltpu.VMEM((ROWS, 4, 8, LANES), f32)
    flat = pltpu.VMEM((ROWS * CHUNKS, LANES), f32)
    dma = pltpu.SemaphoreType.DMA

    def message(count, items, *halves):
        return pltpu.VMEM((*count, items, *halves, width, LANES), f32)

    def in_hbm(block):
        return pltpu.with_memory_space_constraint(lines_of(block), pltpu.HBM)

    rounds = []
    for items in (3, 5):
        rounds += [message((np_,), items), message((np_,), items, 2), message((), items, 2), message((nz,), items, 2)]
    lines, change = pl.pallas_call(
        functools.partial(kernel, nz, plane),
        out_shape=(jax.ShapeDtypeStruct((1024, LANES), f32), jax.ShapeDtypeStruct((1,), f32)),
        in_specs=[anywhere, anywhere],
        out_specs=(in_vmem, in_smem),
        scratch_shapes=[
            flat,
            pltpu.VMEM((ROWS * CHUNKS, LANES), jnp.int32),
            field, field, field, field,
            flat, flat, flat, flat,
            *rounds,
            message((2, np_), 3, 2),
            message((2, np_), 3),
            message((np_,), 4, 2),
            pltpu.VMEM((2, 4, 8, LANES), f32),
            pltpu.VMEM((2, 8, LANES), f32),
            pltpu.VMEM((2, 8, LANES), f32),
            pltpu.VMEM((30, 8, LANES), f32),
            dma((2, 4)),
            dma((2, np_)), dma((2, 2, np_)),
            dma((2, nz)), dma((2, nz)),
            dma((2, 2, np_)), dma((2, np_)),
            dma((2,)), dma((2,)),
        ],
        compiler_params=pltpu.CompilerParams(
            collective_id=0, has_side_effects=True, vmem_limit_bytes=16 * 1024 * 1024
        ),
    )(in_hbm(friction), in_hbm(sources))
    cost, one, two, change = pl.pallas_call(
        finish,
        out_shape=(
            jax.ShapeDtypeStruct((1024, LANES), f32),
            jax.ShapeDtypeStruct((256, LANES), f32),
            jax.ShapeDtypeStruct((64, LANES), f32),
            jax.ShapeDtypeStruct((1,), f32),
        ),
        in_specs=[in_vmem, in_smem],
        out_specs=(anywhere, anywhere, anywhere, in_smem),
        scratch_shapes=[
            flat,
            pltpu.VMEM((512, LANES), f32),
            pltpu.VMEM((24, 4, 8, LANES), f32),
            pltpu.VMEM((256, LANES), f32),
            pltpu.VMEM((64, LANES), f32),
            dma((3,)),
        ],
        compiler_params=pltpu.CompilerParams(vmem_limit_bytes=16 * 1024 * 1024),
    )(lines, change)
    return (block_of(cost, 32), block_of(one, 16), block_of(two, 8), change)


def solution(mesh):
    slabs = mesh.shape["rows"]
    plane = PLANE if slabs >= 32 else (2, 2)
    return jax.shard_map(
        functools.partial(shards, slabs // (plane[0] * plane[1]), plane),
        mesh=mesh,
        in_specs=(P("rows", "cols"), P("rows", "cols")),
        out_specs=(P("rows", "cols"), P("rows", "cols"), P("rows", "cols"), P()),
        check_vma=False,
    )
```

```python
import functools

import jax
import jax.numpy as jnp
from jax import lax
from jax.experimental import pallas as pl
from jax.experimental.pallas import tpu as pltpu
from jax.sharding import PartitionSpec as P

HUGE = 1e30
MESH = pl.DeviceIdType.MESH
ROWS = 32
CHUNKS = 32
LANES = 128
PLANE = (4, 4)
HUB = 1
PARTS = 4
STEPS = LANES // PARTS


def far_first(sizes):
    offsets = [()]
    for size in sizes:
        offsets = [(*o, k) for o in offsets for k in range(size)]
    hops = lambda o: sum(min(k, s - k) for k, s in zip(o, sizes))
    return sorted((o for o in offsets if any(o)), key=hops, reverse=True)


def kernel(
    nz, plane, f_hbm, s_hbm, lines_ref, change_ref,
    fn, sn, h_ref, x_ref, d_ref, u_ref, ht, xt, vf, vb, edge,
    s1a, r1a, s2a, r2a, s1b, r1b, s2b, r2b, s3, r3, pre, enter, xs, xr, paths,
    in_sem, send1, recv1, send2, recv2, send3, recv3, sendx, recvx,
):
    px, py = plane
    np_ = px * py
    width = CHUNKS // np_
    row = lax.axis_index("rows")
    core = lax.axis_index("cols")
    z, p = lax.div(row, np_), lax.rem(row, np_)
    x, y = lax.div(p, py), lax.rem(p, py)
    other_core = 1 - core
    hub = core == HUB
    tile = (4, 8, LANES)
    part = (2, width, LANES)
    near_plane = far_first(plane)
    near_z = far_first((nz,))

    def in_copies(b):
        lines = pl.ds(pl.multiple_of(b * 256, 256), 256)
        return (
            pltpu.make_async_copy(f_hbm.at[lines], fn.at[lines], in_sem.at[0, b]),
            pltpu.make_async_copy(s_hbm.at[lines], sn.at[lines], in_sem.at[1, b]),
        )

    def slot(k):
        dx, dy = near_plane[k]
        return lax.rem(x + dx, px) * py + lax.rem(y + dy, py)

    def z_slot(k):
        return lax.rem(z + near_z[k][0], nz)

    barrier = pltpu.get_barrier_semaphore()

    def greet(device):
        pl.semaphore_signal(barrier, inc=1, device_id=device, device_id_type=MESH)

    for k in range(np_ - 1):
        greet((z * np_ + slot(k), HUB))

    @pl.when(hub)
    def _():
        for k in range(np_ - 1):
            greet((z * np_ + slot(k), 1 - HUB))
        for k in range(nz - 1):
            greet((z_slot(k) * np_ + p, HUB))

    greet((row, other_core))

    for b in range(4):
        for copy in in_copies(b):
            copy.start()

    def wait_for_peers():
        @pl.when(hub)
        def _():
            pl.semaphore_wait(barrier, 2 * (np_ - 1) + nz)

        @pl.when(jnp.logical_not(hub))
        def _():
            pl.semaphore_wait(barrier, np_)

    huge = jnp.full(tile, HUGE, jnp.float32)
    zero = jnp.zeros(tile, jnp.float32)

    def spread(b, _):
        for copy in in_copies(b):
            copy.wait()
        for s in range(8):
            for g in range(4):
                lines = pl.ds((b * 32 + g * 8) * 8 + s, 8, stride=8)
                h_ref[b * 8 + s, g] = 0.5 * fn[lines, :]
                x_ref[b * 8 + s, g] = jnp.where(sn[lines, :] == 1, 0.0, HUGE)
        return 0

    lax.fori_loop(0, ROWS // 8, spread, 0)

    def first_local(b, carry):
        down, up, hd, hu, total = carry
        for s in range(8):
            i = b * 8 + s
            h = h_ref[i]
            down = jnp.minimum(x_ref[i], down + (hd + h))
            total = total + h
            hd = h
            h = h_ref[ROWS - 1 - i]
            up = jnp.minimum(x_ref[ROWS - 1 - i], up + (hu + h))
            hu = h
        return (down, up, hd, hu, total)

    def second_local(b, carry):
        down, up, hd, hu, far_d, far_u, most = carry
        for s in range(8):
            i = b * 8 + s
            h, v = h_ref[i], x_ref[i]
            down = jnp.minimum(v, down + (hd + h))
            far_d = jnp.maximum(v, far_d - (hd + h))
            most = jnp.maximum(most, v - down)
            hd = h
            h, v = h_ref[ROWS - 1 - i], x_ref[ROWS - 1 - i]
            up = jnp.minimum(v, up + (hu + h))
            far_u = jnp.maximum(v, far_u - (hu + h))
            most = jnp.maximum(most, v - up)
            hu = h
        return (down, up, hd, hu, far_d, far_u, most)

    def put(to, item, value):
        for q in range(np_):
            line = q * width
            to[q, item] = value[line // 8, line % 8 : line % 8 + width, :]

    def remote(src, dst, send, recv, device):
        return pltpu.make_async_remote_copy(
            src_ref=src, dst_ref=dst, send_sem=send, recv_sem=recv,
            device_id=device, device_id_type=MESH,
        )

    my_z = jnp.full(part, z, jnp.int32)

    def pick(k, new, old):
        return jnp.where(my_z == k, new, old)

    def vertical(step, window):
        s1, r1, s2, r2 = ((s1a, r1a, s2a, r2a), (s1b, r1b, s2b, r2b))[step]
        if step == 0:
            down, up, hd, hu, total = lax.fori_loop(
                0, ROWS // 8, first_local, (huge, huge, zero, zero, zero)
            )
            values = (up + hu, down + hd, 2.0 * total)
        else:
            down, up, hd, hu, far_d, far_u, most = lax.fori_loop(
                0, ROWS // 8, second_local, (huge, huge, zero, zero, -huge, -huge, zero)
            )
            values = (up + hu, down + hd, far_u - hu, far_d - hd, most)
        items = len(values)
        for item, value in enumerate(values):
            put(s1, item, value)
        if step == 0:
            wait_for_peers()
        copies = []
        for k in range(np_ - 1):
            copy = remote(
                s1.at[slot(k)], r1.at[p, :, core], send1.at[step, k], recv1.at[step, core, k],
                (z * np_ + slot(k), HUB),
            )
            copy.start()
            copies.append(copy)
        last = np_ - 1
        to_hub = remote(
            s1.at[p], r1.at[p, :, core], send1.at[step, last], recv1.at[step, core, last], (row, HUB)
        )

        @pl.when(jnp.logical_not(hub))
        def _():
            to_hub.start()

        window()

        for copy in copies:
            copy.wait_send()

        @pl.when(jnp.logical_not(hub))
        def _():
            to_hub.wait_send()

        to, got = s3.at[step], r3.at[step]

        @pl.when(hub)
        def _():
            for item in range(items):
                r1[p, item, HUB] = s1[p, item]
            for k in range(np_):
                for half in range(2):
                    if k == last and half == HUB:
                        continue
                    remote(
                        s1.at[p], r1.at[p, :, half], send1.at[step, k], recv1.at[step, half, k], (row, HUB)
                    ).wait_recv()
            near = jnp.full(part, HUGE, jnp.float32)
            none = jnp.zeros(part, jnp.float32)
            b, a, s_down, s_up, far_d, far_u, most = near, near, none, none, -near, -near, none
            for q in range(np_):
                r_a, r_b = r1[q, 0], r1[q, 1]
                if step == 0:
                    s = r1[q, 2]
                    pre[q, 2] = s_down
                    s_down = s_down + s
                else:
                    s = r1a[q, 2]
                    most = jnp.maximum(most, jnp.maximum(far_d - r_a, r1[q, 2] - b))
                    most = jnp.maximum(most, r1[q, 4])
                    far_d = jnp.maximum(r1[q, 3], far_d - s)
                pre[q, 0] = b
                b = jnp.minimum(r_b, b + s)
            for q in range(np_ - 1, -1, -1):
                s = r1a[q, 2]
                if step == 0:
                    pre[q, 3] = s_up
                    s_up = s_up + s
                else:
                    far_u = jnp.maximum(r1[q, 2], far_u - s)
                pre[q, 1] = a
                a = jnp.minimum(r1[q, 0], a + s)
            values = (a, b, s_down) if step == 0 else (a, b, far_u, far_d, most)
            for item, value in enumerate(values):
                s2[item] = value
            copies = []
            for k in range(nz - 1):
                copy = remote(
                    s2, r2.at[z], send2.at[step, k], recv2.at[step, k], (z_slot(k) * np_ + p, HUB)
                )
                copy.start()
                copies.append(copy)
            for item in range(items):
                r2[z, item] = values[item]
            for copy in copies:
                copy.wait()

            b, a, far_d, most = near, near, -near, none
            in_d, in_u = near, near
            for k in range(nz):
                in_d = pick(k, b, in_d)
                s = r2a[k, 2]
                if step == 1:
                    most = jnp.maximum(most, jnp.maximum(far_d - r2[k, 0], r2[k, 2] - b))
                    most = jnp.maximum(most, r2[k, 4])
                    far_d = jnp.maximum(r2[k, 3], far_d - s)
                b = jnp.minimum(r2[k, 1], b + s)
            for k in range(nz - 1, -1, -1):
                in_u = pick(k, a, in_u)
                a = jnp.minimum(r2[k, 0], a + r2a[k, 2])
            most = jnp.maximum(most[0], most[1])
            for q in range(np_):
                to[q, 0] = jnp.minimum(pre[q, 0], in_d + pre[q, 2])
                to[q, 1] = jnp.minimum(pre[q, 1], in_u + pre[q, 3])
                to[q, 2, 0] = most
                to[q, 2, 1] = most
            copies = []
            for half in (1 - HUB, HUB):
                for k in range(np_):
                    if k == last and half == HUB:
                        continue
                    q = p if k == last else slot(k)
                    copy = remote(
                        to.at[q, :, half], got.at[p], send3.at[step, half, k], recv3.at[step, k],
                        (z * np_ + q, half),
                    )
                    copy.start()
                    copies.append(copy)
            for item in range(3):
                got[p, item] = to[p, item, HUB]
            for copy in copies:
                copy.wait_send()

        def from_hub(k):
            return remote(
                to.at[p, :, 0], got.at[p], send3.at[step, 0, k], recv3.at[step, k], (row, HUB)
            )

        for k in range(last):
            from_hub(k).wait_recv()

        @pl.when(jnp.logical_not(hub))
        def _():
            from_hub(last).wait_recv()

        most = got[0, 2]
        for q in range(np_):
            line = q * width
            for item in range(2):
                enter[item, line // 8, line % 8 : line % 8 + width, :] = got[q, item]
            most = jnp.maximum(most, got[q, 2])

        def final(b, carry):
            down, up, hd, hu = carry
            for s in range(8):
                i = b * 8 + s
                h = h_ref[i]
                down = jnp.minimum(x_ref[i], down + (hd + h))
                d_ref[i] = down
                hd = h
                h = h_ref[ROWS - 1 - i]
                up = jnp.minimum(x_ref[ROWS - 1 - i], up + (hu + h))
                u_ref[ROWS - 1 - i] = up
                hu = h
            return (down, up, hd, hu)

        lax.fori_loop(0, ROWS // 8, final, (enter[0], enter[1], zero, zero))
        return most

    lane = lax.broadcasted_iota(jnp.int32, (8, LANES), 1)
    sub = lax.broadcasted_iota(jnp.int32, (8, LANES), 0)
    inner, outer = lane % 8, sub % 4
    huge2 = jnp.full((8, LANES), HUGE, jnp.float32)
    zero2 = jnp.zeros((8, LANES), jnp.float32)

    def block(load, j):
        return load(pl.ds((j // 4) * 16, 16), j % 4).reshape(LANES, LANES)

    def at(i):
        return pl.ds(pl.multiple_of(i * 8, 8), 8)

    def chunk_path(shift):
        return paths[11 + shift]

    def group_path(shift):
        return paths[22 + shift]

    def measure():
        for j in range(8):
            ht[pl.ds(j, LANES, stride=8), :] = block(lambda r, g: h_ref[r, g], j).T

        def add(b, sums):
            return tuple(
                sum((ht[at(k * STEPS + b * 8 + s), :] for s in range(8)), start=sums[k])
                for k in range(PARTS)
            )

        sums = lax.fori_loop(0, STEPS // 8, add, (zero2,) * PARTS)
        for k in range(PARTS):
            paths[k] = 2.0 * sums[k]
        whole = 2.0 * (sums[0] + sums[1] + sums[2] + sums[3])
        before = after = zero2
        for k in range(-7, 8):
            rolled = pltpu.roll(whole, k % LANES, 1)
            paths[11 + k] = rolled
            if k > 0:
                before = jnp.where(inner >= k, before + rolled, before)
            if k < 0:
                after = jnp.where(inner - k < 8, after + rolled, after)
        paths[26] = before
        paths[27] = after
        whole = before + whole + after
        before = after = zero2
        for k in range(-3, 4):
            rolled = pltpu.roll(whole, k % 8, 0)
            paths[22 + k] = rolled
            if k > 0:
                before = jnp.where(outer >= k, before + rolled, before)
            if k < 0:
                after = jnp.where(outer - k < 4, after + rolled, after)
        paths[28] = before
        paths[29] = after

        def border(i, path):
            i = core * i + other_core * (LANES - 1 - i)
            h = ht[at(i), :]
            edge[at(i), :] = path + h
            return path + 2.0 * h

        first = jnp.full((8, LANES), core, jnp.int32) == 0
        lax.fori_loop(
            0, LANES, border, jnp.where(first, paths[27] + paths[29], paths[26] + paths[28])
        )

    def scan_all(c, path, axis, size, place, forward):
        step = 1 if forward else -1
        extent = c.shape[axis]
        at_place = place if forward else size - 1 - place
        run = huge2
        for k in range(size - 1, 0, -1):
            ck = pltpu.roll(c, (step * k) % extent, axis)
            run = jnp.where(at_place >= k, jnp.minimum(ck, run + path(step * k)), run)
        before = run
        run = jnp.minimum(c, run + path(0))
        for k in range(1, size):
            ck = pltpu.roll(c, (-step * k) % extent, axis)
            run = jnp.where(at_place + k < size, jnp.minimum(ck, run + path(-step * k)), run)
        return before, run

    def horizontal(step, window):
        for j in range(8):
            rows = pl.ds(j, LANES, stride=8)
            xt[rows, :] = block(lambda r, g: jnp.minimum(d_ref[r, g], u_ref[r, g]), j).T

        def sweep(start_f, start_b, store):
            def some(b, carry):
                right, left, hr, hl = (list(c) for c in carry)
                for s in range(8):
                    for k in range(PARTS):
                        i = k * STEPS + b * 8 + s
                        h = ht[at(i), :]
                        right[k] = jnp.minimum(xt[at(i), :], right[k] + (hr[k] + h))
                        if store:
                            vf[at(i), :] = right[k]
                        hr[k] = h
                        i = (k + 1) * STEPS - 1 - (b * 8 + s)
                        h = ht[at(i), :]
                        left[k] = jnp.minimum(xt[at(i), :], left[k] + (hl[k] + h))
                        if store:
                            vb[at(i), :] = left[k]
                        hl[k] = h
                return (tuple(right), tuple(left), tuple(hr), tuple(hl))

            zeros = (zero2,) * PARTS
            return lax.fori_loop(0, STEPS // 8, some, (start_f, start_b, zeros, zeros))

        right, left, hr, hl = sweep((huge2,) * PARTS, (huge2,) * PARTS, False)
        right = [r + h for r, h in zip(right, hr)]
        left = [r + h for r, h in zip(left, hl)]
        c_f, c_b = right[0], left[-1]
        for k in range(1, PARTS):
            c_f = jnp.minimum(right[k], c_f + paths[k])
            c_b = jnp.minimum(left[-1 - k], c_b + paths[PARTS - 1 - k])
        fc, f_all = scan_all(c_f, chunk_path, 1, 8, inner, True)
        bc, b_all = scan_all(c_b, chunk_path, 1, 8, inner, False)
        gfc, gf_all = scan_all(f_all, group_path, 0, 4, outer, True)
        gbc, gb_all = scan_all(b_all, group_path, 0, 4, outer, False)
        first = jnp.full((8, LANES), core, jnp.int32) == 0
        xs[step] = jnp.where(first, gf_all, gb_all)
        copy = remote(xs.at[step], xr.at[step], sendx.at[step], recvx.at[step], (row, other_core))
        copy.start()
        in_f = [jnp.minimum(fc, gfc + paths[26])]
        in_b = [jnp.minimum(bc, gbc + paths[27])]
        for k in range(PARTS - 1):
            in_f.append(jnp.minimum(right[k], in_f[k] + paths[k]))
            in_b.append(jnp.minimum(left[-1 - k], in_b[k] + paths[PARTS - 1 - k]))
        sweep(tuple(in_f), tuple(in_b[::-1]), True)
        window()
        copy.wait()
        return xr[step]

    def in_row(other, j):
        rows = pl.ds(j, LANES, stride=8)
        return jnp.minimum(jnp.minimum(vf[rows, :], vb[rows, :]), edge[rows, :] + other[j : j + 1])

    vertical(0, measure)
    other = horizontal(0, lambda: None)
    for j in range(8):
        back = in_row(other, j).T
        x_ref[pl.ds((j // 4) * 16, 16), j % 4] = back.reshape(16, 8, LANES)
    most = vertical(1, lambda: None)

    def reduce_change():
        change_ref[0] = jnp.max(most)

    other = horizontal(1, reduce_change)

    def merge(b, _):
        for t in range(16):
            i = at(b * 16 + t)
            lines_ref[i, :] = jnp.minimum(jnp.minimum(vf[i, :], vb[i, :]), edge[i, :] + other)
        return 0

    lax.fori_loop(0, 8, merge, 0)


def finish(xt, most, cost_hbm, one_hbm, two_hbm, change_ref, on, pairs, pool, o1, o2, out_sem):
    lane = lax.broadcasted_iota(jnp.int32, (8, LANES), 1)
    outs = []
    for j in range(8):
        back = xt[pl.ds(j, LANES, stride=8), :].T
        for r in range(16):
            i = (j // 4) * 16 + r
            lines = pl.ds(((i // 8) * 32 + (j % 4) * 8) * 8 + i % 8, 8, stride=8)
            on[lines, :] = back[r * 8 : (r + 1) * 8, :]
        if j % 4 == 3:
            half = pl.ds((j // 4) * 512, 512)
            outs.append(pltpu.make_async_copy(on.at[half], cost_hbm.at[half], out_sem.at[2 + j // 4]))
            outs[-1].start()

    for j in range(8):
        pair = jnp.minimum(xt[pl.ds(j, 64, stride=16), :], xt[pl.ds(j + 8, 64, stride=16), :])
        lines = jnp.concatenate([pair, pair], axis=0).T.reshape(8, 2, 8, LANES)
        pool[pl.ds((j // 4) * 8, 8), j % 4] = jnp.minimum(lines[:, 0], lines[:, 1])
        pairs[pl.ds(j, 64, stride=8), :] = pair
    for a in range(16):
        for g in range(2):
            halves = [
                jnp.concatenate([pool[a, 2 * g + t, pl.ds(i, 4, stride=2), :] for t in range(2)], axis=0)
                for i in range(2)
            ]
            lines = pl.ds(((a // 8) * 16 + g * 8) * 8 + a % 8, 8, stride=8)
            o1[lines, :] = jnp.where(lane < 64, halves[0], halves[1])
    out_one = pltpu.make_async_copy(o1, one_hbm, out_sem.at[0])
    out_one.start()

    for j in range(8):
        quad = jnp.minimum(pairs[pl.ds(j, 32, stride=16), :], pairs[pl.ds(j + 8, 32, stride=16), :])
        lines = jnp.concatenate([quad] * 4, axis=0).T.reshape(4, 4, 8, LANES)
        lines = jnp.minimum(
            jnp.minimum(lines[:, 0], lines[:, 1]), jnp.minimum(lines[:, 2], lines[:, 3])
        )
        pool[pl.ds(16 + (j // 4) * 4, 4), j % 4] = lines
    for a in range(8):
        quarters = [
            jnp.concatenate([pool[16 + a, g, pl.ds(i, 2, stride=4), :] for g in range(4)], axis=0)
            for i in range(4)
        ]
        low = jnp.where(lane < 32, quarters[0], quarters[1])
        high = jnp.where(lane < 96, quarters[2], quarters[3])
        o2[pl.ds(a, 8, stride=8), :] = jnp.where(lane < 64, low, high)
    out_two = pltpu.make_async_copy(o2, two_hbm, out_sem.at[1])
    out_two.start()
    change_ref[0] = most[0]
    for out in outs:
        out.wait()
    out_one.wait()
    out_two.wait()


def lines_of(block):
    height, length = block.shape
    return (
        block.reshape(height // 8, 8, length // LANES, LANES)
        .transpose(0, 2, 1, 3)
        .reshape(-1, LANES)
    )


def block_of(lines, height):
    return lines.reshape(height // 8, -1, 8, LANES).transpose(0, 2, 1, 3).reshape(height, -1)


def shards(nz, plane, friction, sources):
    np_ = plane[0] * plane[1]
    width = CHUNKS // np_
    f32 = jnp.float32
    anywhere = pl.BlockSpec(memory_space=pltpu.HBM)
    in_vmem = pl.BlockSpec(memory_space=pltpu.VMEM)
    in_smem = pl.BlockSpec(memory_space=pltpu.SMEM)
    field = pltpu.VMEM((ROWS, 4, 8, LANES), f32)
    flat = pltpu.VMEM((ROWS * CHUNKS, LANES), f32)
    dma = pltpu.SemaphoreType.DMA

    def message(count, items, *halves):
        return pltpu.VMEM((*count, items, *halves, width, LANES), f32)

    def in_hbm(block):
        return pltpu.with_memory_space_constraint(lines_of(block), pltpu.HBM)

    rounds = []
    for items in (3, 5):
        rounds += [message((np_,), items), message((np_,), items, 2), message((), items, 2), message((nz,), items, 2)]
    lines, change = pl.pallas_call(
        functools.partial(kernel, nz, plane),
        out_shape=(jax.ShapeDtypeStruct((1024, LANES), f32), jax.ShapeDtypeStruct((1,), f32)),
        in_specs=[anywhere, anywhere],
        out_specs=(in_vmem, in_smem),
        scratch_shapes=[
            flat,
            pltpu.VMEM((ROWS * CHUNKS, LANES), jnp.int32),
            field, field, field, field,
            flat, flat, flat, flat, flat,
            *rounds,
            message((2, np_), 3, 2),
            message((2, np_), 3),
            message((np_,), 4, 2),
            pltpu.VMEM((2, 4, 8, LANES), f32),
            pltpu.VMEM((2, 8, LANES), f32),
            pltpu.VMEM((2, 8, LANES), f32),
            pltpu.VMEM((30, 8, LANES), f32),
            dma((2, 4)),
            dma((2, np_)), dma((2, 2, np_)),
            dma((2, nz)), dma((2, nz)),
            dma((2, 2, np_)), dma((2, np_)),
            dma((2,)), dma((2,)),
        ],
        compiler_params=pltpu.CompilerParams(
            collective_id=0, has_side_effects=True, vmem_limit_bytes=16 * 1024 * 1024
        ),
    )(in_hbm(friction), in_hbm(sources))
    cost, one, two, change = pl.pallas_call(
        finish,
        out_shape=(
            jax.ShapeDtypeStruct((1024, LANES), f32),
            jax.ShapeDtypeStruct((256, LANES), f32),
            jax.ShapeDtypeStruct((64, LANES), f32),
            jax.ShapeDtypeStruct((1,), f32),
        ),
        in_specs=[in_vmem, in_smem],
        out_specs=(anywhere, anywhere, anywhere, in_smem),
        scratch_shapes=[
            flat,
            pltpu.VMEM((512, LANES), f32),
            pltpu.VMEM((24, 4, 8, LANES), f32),
            pltpu.VMEM((256, LANES), f32),
            pltpu.VMEM((64, LANES), f32),
            dma((4,)),
        ],
        compiler_params=pltpu.CompilerParams(vmem_limit_bytes=16 * 1024 * 1024),
    )(lines, change)
    return (block_of(cost, 32), block_of(one, 16), block_of(two, 8), change)


def solution(mesh):
    slabs = mesh.shape["rows"]
    plane = PLANE if slabs >= 32 else (2, 2)
    return jax.shard_map(
        functools.partial(shards, slabs // (plane[0] * plane[1]), plane),
        mesh=mesh,
        in_specs=(P("rows", "cols"), P("rows", "cols")),
        out_specs=(P("rows", "cols"), P("rows", "cols"), P("rows", "cols"), P()),
        check_vma=False,
    )
```

```python
import functools

import jax
import jax.numpy as jnp
from jax import lax
from jax.experimental import pallas as pl
from jax.experimental.pallas import tpu as pltpu
from jax.sharding import PartitionSpec as P

HUGE = 1e30
MESH = pl.DeviceIdType.MESH
ROWS = 32
CHUNKS = 32
LANES = 128
PLANE = (4, 4)
HUB = 1
PARTS = 4
STEPS = LANES // PARTS


def far_first(sizes):
    offsets = [()]
    for size in sizes:
        offsets = [(*o, k) for o in offsets for k in range(size)]
    hops = lambda o: sum(min(k, s - k) for k, s in zip(o, sizes))
    return sorted((o for o in offsets if any(o)), key=hops, reverse=True)


def kernel(
    nz, plane, f_hbm, s_hbm, lines_ref, most_ref,
    fn, sn, h_ref, x_ref, d_ref, u_ref, ht, xt, vf, vb, edge,
    s1a, r1a, s1b, r1b, s1c, r1c, s2a, r2a, s2b, r2b, s2c, r2c, s3, r3, s3c, r3c, pre, enter, xs, xr, paths,
    in_sem, send1, recv1, send2, recv2, send3, recv3, sendx, recvx,
):
    px, py = plane
    np_ = px * py
    width = CHUNKS // np_
    row = lax.axis_index("rows")
    core = lax.axis_index("cols")
    z, p = lax.div(row, np_), lax.rem(row, np_)
    x, y = lax.div(p, py), lax.rem(p, py)
    other_core = 1 - core
    hub = core == HUB
    tile = (4, 8, LANES)
    part = (2, width, LANES)
    near_plane = far_first(plane)
    near_z = far_first((nz,))

    def in_copies(b):
        lines = pl.ds(pl.multiple_of(b * 256, 256), 256)
        return (
            pltpu.make_async_copy(f_hbm.at[lines], fn.at[lines], in_sem.at[0, b]),
            pltpu.make_async_copy(s_hbm.at[lines], sn.at[lines], in_sem.at[1, b]),
        )

    x_at = [x] + [lax.rem(x + d, px) for d in range(1, px)]
    y_at = [y] + [lax.rem(y + d, py) for d in range(1, py)]
    z_at = [z] + [lax.rem(z + d, nz) for d in range(1, nz)]

    def slot(k):
        dx, dy = near_plane[k]
        return x_at[dx] * py + y_at[dy]

    def z_slot(k):
        return z_at[near_z[k][0]]

    barrier = pltpu.get_barrier_semaphore()

    def greet(device):
        pl.semaphore_signal(barrier, inc=1, device_id=device, device_id_type=MESH)

    for k in range(np_ - 1):
        greet((z * np_ + slot(k), HUB))

    @pl.when(hub)
    def _():
        for k in range(np_ - 1):
            greet((z * np_ + slot(k), 1 - HUB))
        for k in range(nz - 1):
            greet((z_slot(k) * np_ + p, HUB))

    greet((row, other_core))

    for b in range(4):
        for copy in in_copies(b):
            copy.start()

    def wait_for_peers():
        @pl.when(hub)
        def _():
            pl.semaphore_wait(barrier, 2 * (np_ - 1) + nz)

        @pl.when(jnp.logical_not(hub))
        def _():
            pl.semaphore_wait(barrier, np_)

    huge = jnp.full(tile, HUGE, jnp.float32)
    zero = jnp.zeros(tile, jnp.float32)

    def spread(b, _):
        for copy in in_copies(b):
            copy.wait()
        for s in range(8):
            for g in range(4):
                lines = pl.ds((b * 32 + g * 8) * 8 + s, 8, stride=8)
                h_ref[b * 8 + s, g] = 0.5 * fn[lines, :]
                x_ref[b * 8 + s, g] = jnp.where(sn[lines, :] == 1, 0.0, HUGE)
        return 0

    lax.fori_loop(0, ROWS // 8, spread, 0)

    def border_costs(b, carry):
        down, up, hd, hu = carry
        for s in range(8):
            i = b * 8 + s
            h = h_ref[i]
            down = jnp.minimum(x_ref[i], down + (hd + h))
            hd = h
            h = h_ref[ROWS - 1 - i]
            up = jnp.minimum(x_ref[ROWS - 1 - i], up + (hu + h))
            hu = h
        return (down, up, hd, hu)

    def add_rows(b, total):
        return sum((h_ref[b * 8 + s] for s in range(8)), start=total)

    def second_local(b, carry):
        down, up, hd, hu, far_d, far_u, most = carry
        for s in range(8):
            i = b * 8 + s
            h, v = h_ref[i], x_ref[i]
            down = jnp.minimum(v, down + (hd + h))
            far_d = jnp.maximum(v, far_d - (hd + h))
            most = jnp.maximum(most, v - down)
            hd = h
            h, v = h_ref[ROWS - 1 - i], x_ref[ROWS - 1 - i]
            up = jnp.minimum(v, up + (hu + h))
            far_u = jnp.maximum(v, far_u - (hu + h))
            most = jnp.maximum(most, v - up)
            hu = h
        return (down, up, hd, hu, far_d, far_u, most)

    def put(to, item, value):
        for q in range(np_):
            line = q * width
            to[q, item] = value[line // 8, line % 8 : line % 8 + width, :]

    def remote(src, dst, send, recv, device):
        return pltpu.make_async_remote_copy(
            src_ref=src, dst_ref=dst, send_sem=send, recv_sem=recv,
            device_id=device, device_id_type=MESH,
        )

    my_z = jnp.full(part, z, jnp.int32)
    last = np_ - 1
    not_hub = jnp.logical_not(hub)

    def to_hub(to, got, n, k):
        q = p if k == last else slot(k)
        return remote(
            to.at[q], got.at[core, p], send1.at[n, k], recv1.at[n, core, k], (z * np_ + q, HUB)
        )

    def send_to_hubs(to, got, n):
        for k in range(last):
            to_hub(to, got, n, k).start()

        @pl.when(not_hub)
        def _():
            to_hub(to, got, n, last).start()

    def sent_to_hubs(to, got, n):
        for k in range(last):
            to_hub(to, got, n, k).wait_send()

        @pl.when(not_hub)
        def _():
            to_hub(to, got, n, last).wait_send()

    def hub_has(to, got, n):
        for item in range(to.shape[1]):
            got[HUB, p, item] = to[p, item]
        for k in range(np_ - 1, -1, -1):
            for half in range(2):
                if k == last and half == HUB:
                    continue
                remote(
                    to.at[p], got.at[half, p], send1.at[n, k], recv1.at[n, half, k], (row, HUB)
                ).wait_recv()

    def along_z(source, got, n, k):
        return remote(
            source(k), got.at[z], send2.at[n, k], recv2.at[n, k], (z_slot(k) * np_ + p, HUB)
        )

    def by_side(to):
        return lambda k: to.at[lax.div(z_slot(k) - z + nz, nz)]

    def from_hub(source, got, n, half, k):
        q = p if k == last else slot(k)
        return remote(
            source(half, q), got.at[p], send3.at[n, half, k], recv3.at[n, k], (z * np_ + q, half)
        )

    to_cores = [(half, k) for half in (1 - HUB, HUB) for k in range(np_) if (half, k) != (HUB, last)]

    def cores_have(got, n):
        def copy(k):
            return remote(got.at[p], got.at[p], send3.at[n, HUB, k], recv3.at[n, k], (row, HUB))

        @pl.when(not_hub)
        def _():
            copy(last).wait_recv()

        for k in range(last - 1, -1, -1):
            copy(k).wait_recv()

    def plain(ref):
        return lambda *_: ref

    near = jnp.full(part, HUGE, jnp.float32)
    none = jnp.zeros(part, jnp.float32)
    rounds = ((s1a, r1a, s2a, r2a), (s1b, r1b, s2b, r2b))

    def vertical(step, window):
        s1, r1, s2, r2 = rounds[step]
        down, up, hd, hu = lax.fori_loop(0, ROWS // 8, border_costs, (huge, huge, zero, zero))
        put(s1, 0, up + hu)
        put(s1, 1, down + hd)
        if step == 0:
            put(s1, 2, 2.0 * lax.fori_loop(0, ROWS // 8, add_rows, zero))
            wait_for_peers()
        send_to_hubs(s1, r1, step)
        window()
        to, got = s3.at[step], r3.at[step]

        @pl.when(hub)
        def _():
            hub_has(s1, r1, step)
            b, a, s_down, s_up = near, near, none, none
            for q in range(np_):
                s = r1a[:, q, 2]
                if step == 0:
                    pre[q, 2] = s_down
                    s_down = s_down + s
                pre[q, 0] = b
                b = jnp.minimum(r1[:, q, 1], b + s)
            for q in range(np_ - 1, -1, -1):
                s = r1a[:, q, 2]
                if step == 0:
                    pre[q, 3] = s_up
                    s_up = s_up + s
                pre[q, 1] = a
                a = jnp.minimum(r1[:, q, 0], a + s)
            for side, value in enumerate((a, b)):
                s2[side, 0] = value
                if step == 0:
                    s2[side, 1] = s_down
            for k in range(nz - 1):
                along_z(by_side(s2), r2, step, k).start()
            r2[z, 0] = b
            if step == 0:
                r2[z, 1] = s_down
            else:
                hub_has(s1c, r1c, 2)
                b, far_d, far_u, most = near, -near, -near, none
                for q in range(np_):
                    s, r_p = r1a[:, q, 2], r1c[:, q, 0]
                    most = jnp.maximum(most, jnp.maximum(far_d - r1[:, q, 0], r_p - b))
                    most = jnp.maximum(most, r1c[:, q, 2])
                    far_d = jnp.maximum(r1c[:, q, 1], far_d - s)
                    b = jnp.minimum(r1[:, q, 1], b + s)
                for q in range(np_ - 1, -1, -1):
                    far_u = jnp.maximum(r1c[:, q, 0], far_u - r1a[:, q, 2])
                for item, value in enumerate((a, b, far_u, far_d, most)):
                    s2c[item] = value
                    r2c[z, item] = value
                for k in range(nz - 1):
                    along_z(plain(s2c), r2c, 2, k).start()
            for k in range(nz - 2, -1, -1):
                along_z(by_side(s2), r2, step, k).wait_recv()
            in_d, in_u = near, near
            for k in range(nz):
                in_d = jnp.where(my_z > k, jnp.minimum(r2[k, 0], in_d + r2a[k, 1]), in_d)
            for k in range(nz - 1, -1, -1):
                in_u = jnp.where(my_z < k, jnp.minimum(r2[k, 0], in_u + r2a[k, 1]), in_u)
            for q in range(np_):
                to[:, q, 0] = jnp.minimum(pre[q, 0], in_d + pre[q, 2])
                to[:, q, 1] = jnp.minimum(pre[q, 1], in_u + pre[q, 3])
            for half, k in to_cores:
                from_hub(lambda h, q: to.at[h, q], got, step, half, k).start()
            for item in range(2):
                got[p, item] = to[HUB, p, item]
            if step == 1:
                for k in range(nz - 2, -1, -1):
                    along_z(plain(s2c), r2c, 2, k).wait_recv()
                b, far_d, most = near, -near, none
                for k in range(nz):
                    s = r2a[k, 1]
                    most = jnp.maximum(most, jnp.maximum(far_d - r2c[k, 0], r2c[k, 2] - b))
                    most = jnp.maximum(most, r2c[k, 4])
                    far_d = jnp.maximum(r2c[k, 3], far_d - s)
                    b = jnp.minimum(r2c[k, 1], b + s)
                most = jnp.maximum(most[0], most[1])
                s3c[...] = most
                r3c[p] = most
                for half, k in to_cores:
                    from_hub(plain(s3c), r3c, 2, half, k).start()

        cores_have(got, step)
        for q in range(np_):
            line = q * width
            for item in range(2):
                enter[item, line // 8, line % 8 : line % 8 + width, :] = got[q, item]

        def final(b, carry):
            down, up, hd, hu = carry
            for s in range(8):
                i = b * 8 + s
                h = h_ref[i]
                down = jnp.minimum(x_ref[i], down + (hd + h))
                d_ref[i] = down
                hd = h
                h = h_ref[ROWS - 1 - i]
                up = jnp.minimum(x_ref[ROWS - 1 - i], up + (hu + h))
                u_ref[ROWS - 1 - i] = up
                hu = h
            return (down, up, hd, hu)

        lax.fori_loop(0, ROWS // 8, final, (enter[0], enter[1], zero, zero))

    def second_window():
        _, _, hd, hu, far_d, far_u, most = lax.fori_loop(
            0, ROWS // 8, second_local, (huge, huge, zero, zero, -huge, -huge, zero)
        )
        put(s1c, 0, far_u - hu)
        put(s1c, 1, far_d - hd)
        put(s1c, 2, most)
        send_to_hubs(s1c, r1c, 2)

    def drain(step):
        s1, r1, s2, r2 = rounds[step]
        sent_to_hubs(s1, r1, step)
        to, got = s3.at[step], r3.at[step]
        if step == 1:
            sent_to_hubs(s1c, r1c, 2)
            cores_have(r3c, 2)

        @pl.when(hub)
        def _():
            for k in range(nz - 1):
                along_z(by_side(s2), r2, step, k).wait_send()
                if step == 1:
                    along_z(plain(s2c), r2c, 2, k).wait_send()
            for half, k in to_cores:
                from_hub(lambda h, q: to.at[h, q], got, step, half, k).wait_send()
                if step == 1:
                    from_hub(plain(s3c), r3c, 2, half, k).wait_send()

    lane = lax.broadcasted_iota(jnp.int32, (8, LANES), 1)
    sub = lax.broadcasted_iota(jnp.int32, (8, LANES), 0)
    inner, outer = lane % 8, sub % 4
    huge2 = jnp.full((8, LANES), HUGE, jnp.float32)
    zero2 = jnp.zeros((8, LANES), jnp.float32)

    def block(load, j):
        return load(pl.ds((j // 4) * 16, 16), j % 4).reshape(LANES, LANES)

    def at(i):
        return pl.ds(pl.multiple_of(i * 8, 8), 8)

    def chunk_path(shift):
        return paths[11 + shift]

    def group_path(shift):
        return paths[22 + shift]

    def measure():
        for j in range(8):
            ht[pl.ds(j, LANES, stride=8), :] = block(lambda r, g: h_ref[r, g], j).T

        def add(b, sums):
            return tuple(
                sum((ht[at(k * STEPS + b * 8 + s), :] for s in range(8)), start=sums[k])
                for k in range(PARTS)
            )

        sums = lax.fori_loop(0, STEPS // 8, add, (zero2,) * PARTS)
        for k in range(PARTS):
            paths[k] = 2.0 * sums[k]
        whole = 2.0 * (sums[0] + sums[1] + sums[2] + sums[3])
        before = after = zero2
        for k in range(-7, 8):
            rolled = pltpu.roll(whole, k % LANES, 1)
            paths[11 + k] = rolled
            if k > 0:
                before = jnp.where(inner >= k, before + rolled, before)
            if k < 0:
                after = jnp.where(inner - k < 8, after + rolled, after)
        paths[26] = before
        paths[27] = after
        whole = before + whole + after
        before = after = zero2
        for k in range(-3, 4):
            rolled = pltpu.roll(whole, k % 8, 0)
            paths[22 + k] = rolled
            if k > 0:
                before = jnp.where(outer >= k, before + rolled, before)
            if k < 0:
                after = jnp.where(outer - k < 4, after + rolled, after)
        paths[28] = before
        paths[29] = after

        def border(i, path):
            i = core * i + other_core * (LANES - 1 - i)
            h = ht[at(i), :]
            edge[at(i), :] = path + h
            return path + 2.0 * h

        first = jnp.full((8, LANES), core, jnp.int32) == 0
        lax.fori_loop(
            0, LANES, border, jnp.where(first, paths[27] + paths[29], paths[26] + paths[28])
        )

    def scan_all(c, path, axis, size, place, forward):
        step = 1 if forward else -1
        extent = c.shape[axis]
        at_place = place if forward else size - 1 - place
        run = huge2
        for k in range(size - 1, 0, -1):
            ck = pltpu.roll(c, (step * k) % extent, axis)
            run = jnp.where(at_place >= k, jnp.minimum(ck, run + path(step * k)), run)
        before = run
        run = jnp.minimum(c, run + path(0))
        for k in range(1, size):
            ck = pltpu.roll(c, (-step * k) % extent, axis)
            run = jnp.where(at_place + k < size, jnp.minimum(ck, run + path(-step * k)), run)
        return before, run

    def horizontal(step, window):
        for j in range(8):
            rows = pl.ds(j, LANES, stride=8)
            xt[rows, :] = block(lambda r, g: jnp.minimum(d_ref[r, g], u_ref[r, g]), j).T

        def sweep(start_f, start_b, store):
            def some(b, carry):
                right, left, hr, hl = (list(c) for c in carry)
                for s in range(8):
                    for k in range(PARTS):
                        i = k * STEPS + b * 8 + s
                        h = ht[at(i), :]
                        right[k] = jnp.minimum(xt[at(i), :], right[k] + (hr[k] + h))
                        if store:
                            vf[at(i), :] = right[k]
                        hr[k] = h
                        i = (k + 1) * STEPS - 1 - (b * 8 + s)
                        h = ht[at(i), :]
                        left[k] = jnp.minimum(xt[at(i), :], left[k] + (hl[k] + h))
                        if store:
                            vb[at(i), :] = left[k]
                        hl[k] = h
                return (tuple(right), tuple(left), tuple(hr), tuple(hl))

            zeros = (zero2,) * PARTS
            return lax.fori_loop(0, STEPS // 8, some, (start_f, start_b, zeros, zeros))

        right, left, hr, hl = sweep((huge2,) * PARTS, (huge2,) * PARTS, False)
        right = [r + h for r, h in zip(right, hr)]
        left = [r + h for r, h in zip(left, hl)]
        c_f, c_b = right[0], left[-1]
        for k in range(1, PARTS):
            c_f = jnp.minimum(right[k], c_f + paths[k])
            c_b = jnp.minimum(left[-1 - k], c_b + paths[PARTS - 1 - k])
        fc, f_all = scan_all(c_f, chunk_path, 1, 8, inner, True)
        bc, b_all = scan_all(c_b, chunk_path, 1, 8, inner, False)
        gfc, gf_all = scan_all(f_all, group_path, 0, 4, outer, True)
        gbc, gb_all = scan_all(b_all, group_path, 0, 4, outer, False)
        first = jnp.full((8, LANES), core, jnp.int32) == 0
        xs[step] = jnp.where(first, gf_all, gb_all)
        copy = remote(xs.at[step], xr.at[step], sendx.at[step], recvx.at[step], (row, other_core))
        copy.start()
        in_f = [jnp.minimum(fc, gfc + paths[26])]
        in_b = [jnp.minimum(bc, gbc + paths[27])]
        for k in range(PARTS - 1):
            in_f.append(jnp.minimum(right[k], in_f[k] + paths[k]))
            in_b.append(jnp.minimum(left[-1 - k], in_b[k] + paths[PARTS - 1 - k]))
        sweep(tuple(in_f), tuple(in_b[::-1]), True)
        window()
        copy.wait()
        return xr[step]

    def in_row(other, j):
        rows = pl.ds(j, LANES, stride=8)
        return jnp.minimum(jnp.minimum(vf[rows, :], vb[rows, :]), edge[rows, :] + other[j : j + 1])

    vertical(0, measure)
    other = horizontal(0, lambda: drain(0))
    for j in range(8):
        back = in_row(other, j).T
        x_ref[pl.ds((j // 4) * 16, 16), j % 4] = back.reshape(16, 8, LANES)
    vertical(1, second_window)
    other = horizontal(1, lambda: drain(1))
    most = r3c[0]
    for q in range(1, np_):
        most = jnp.maximum(most, r3c[q])
    most_ref[...] = most

    def merge(b, _):
        for t in range(16):
            i = at(b * 16 + t)
            lines_ref[i, :] = jnp.minimum(jnp.minimum(vf[i, :], vb[i, :]), edge[i, :] + other)
        return 0

    lax.fori_loop(0, 8, merge, 0)


def finish(xt, most, cost_hbm, one_hbm, two_hbm, change_hbm, on, pairs, pool, o1, o2, change, out_sem):
    lane = lax.broadcasted_iota(jnp.int32, (8, LANES), 1)
    change[0] = jnp.max(most[...])
    outs = [pltpu.make_async_copy(change, change_hbm, out_sem.at[4])]
    outs[0].start()
    for j in range(8):
        back = xt[pl.ds(j, LANES, stride=8), :].T
        for r in range(16):
            i = (j // 4) * 16 + r
            lines = pl.ds(((i // 8) * 32 + (j % 4) * 8) * 8 + i % 8, 8, stride=8)
            on[lines, :] = back[r * 8 : (r + 1) * 8, :]
        if j % 4 == 3:
            half = pl.ds((j // 4) * 512, 512)
            outs.append(pltpu.make_async_copy(on.at[half], cost_hbm.at[half], out_sem.at[2 + j // 4]))
            outs[-1].start()

    for j in range(8):
        pair = jnp.minimum(xt[pl.ds(j, 64, stride=16), :], xt[pl.ds(j + 8, 64, stride=16), :])
        lines = jnp.concatenate([pair, pair], axis=0).T.reshape(8, 2, 8, LANES)
        pool[pl.ds((j // 4) * 8, 8), j % 4] = jnp.minimum(lines[:, 0], lines[:, 1])
        pairs[pl.ds(j, 64, stride=8), :] = pair
    for a in range(16):
        for g in range(2):
            halves = [
                jnp.concatenate([pool[a, 2 * g + t, pl.ds(i, 4, stride=2), :] for t in range(2)], axis=0)
                for i in range(2)
            ]
            lines = pl.ds(((a // 8) * 16 + g * 8) * 8 + a % 8, 8, stride=8)
            o1[lines, :] = jnp.where(lane < 64, halves[0], halves[1])
    out_one = pltpu.make_async_copy(o1, one_hbm, out_sem.at[0])
    out_one.start()

    for j in range(8):
        quad = jnp.minimum(pairs[pl.ds(j, 32, stride=16), :], pairs[pl.ds(j + 8, 32, stride=16), :])
        lines = jnp.concatenate([quad] * 4, axis=0).T.reshape(4, 4, 8, LANES)
        lines = jnp.minimum(
            jnp.minimum(lines[:, 0], lines[:, 1]), jnp.minimum(lines[:, 2], lines[:, 3])
        )
        pool[pl.ds(16 + (j // 4) * 4, 4), j % 4] = lines
    for a in range(8):
        quarters = [
            jnp.concatenate([pool[16 + a, g, pl.ds(i, 2, stride=4), :] for g in range(4)], axis=0)
            for i in range(4)
        ]
        low = jnp.where(lane < 32, quarters[0], quarters[1])
        high = jnp.where(lane < 96, quarters[2], quarters[3])
        o2[pl.ds(a, 8, stride=8), :] = jnp.where(lane < 64, low, high)
    out_two = pltpu.make_async_copy(o2, two_hbm, out_sem.at[1])
    out_two.start()
    for out in outs:
        out.wait()
    out_one.wait()
    out_two.wait()


def lines_of(block):
    height, length = block.shape
    return (
        block.reshape(height // 8, 8, length // LANES, LANES)
        .transpose(0, 2, 1, 3)
        .reshape(-1, LANES)
    )


def block_of(lines, height):
    return lines.reshape(height // 8, -1, 8, LANES).transpose(0, 2, 1, 3).reshape(height, -1)


def shards(nz, plane, friction, sources):
    np_ = plane[0] * plane[1]
    width = CHUNKS // np_
    f32 = jnp.float32
    anywhere = pl.BlockSpec(memory_space=pltpu.HBM)
    in_vmem = pl.BlockSpec(memory_space=pltpu.VMEM)
    field = pltpu.VMEM((ROWS, 4, 8, LANES), f32)
    flat = pltpu.VMEM((ROWS * CHUNKS, LANES), f32)
    dma = pltpu.SemaphoreType.DMA

    def message(count, items, *halves):
        return pltpu.VMEM((*count, items, *halves, width, LANES), f32)

    def in_hbm(block):
        return pltpu.with_memory_space_constraint(lines_of(block), pltpu.HBM)

    rounds = []
    for items in (3, 2, 3):
        rounds += [message((np_,), items), message((2, np_), items)]
    for sides, items in (((2,), 2), ((2,), 1), ((), 5)):
        rounds += [message(sides, items, 2), message((nz,), items, 2)]
    lines, most = pl.pallas_call(
        functools.partial(kernel, nz, plane),
        out_shape=(jax.ShapeDtypeStruct((1024, LANES), f32), jax.ShapeDtypeStruct((width, LANES), f32)),
        in_specs=[anywhere, anywhere],
        out_specs=(in_vmem, in_vmem),
        scratch_shapes=[
            flat,
            pltpu.VMEM((ROWS * CHUNKS, LANES), jnp.int32),
            field, field, field, field,
            flat, flat, flat, flat, flat,
            *rounds,
            message((2, 2, np_), 2),
            message((2, np_), 2),
            pltpu.VMEM((width, LANES), f32),
            pltpu.VMEM((np_, width, LANES), f32),
            message((np_,), 4, 2),
            pltpu.VMEM((2, 4, 8, LANES), f32),
            pltpu.VMEM((2, 8, LANES), f32),
            pltpu.VMEM((2, 8, LANES), f32),
            pltpu.VMEM((30, 8, LANES), f32),
            dma((2, 4)),
            dma((3, np_)), dma((3, 2, np_)),
            dma((3, nz)), dma((3, nz)),
            dma((3, 2, np_)), dma((3, np_)),
            dma((2,)), dma((2,)),
        ],
        compiler_params=pltpu.CompilerParams(
            collective_id=0, has_side_effects=True, vmem_limit_bytes=16 * 1024 * 1024
        ),
    )(in_hbm(friction), in_hbm(sources))
    cost, one, two, change = pl.pallas_call(
        finish,
        out_shape=(
            jax.ShapeDtypeStruct((1024, LANES), f32),
            jax.ShapeDtypeStruct((256, LANES), f32),
            jax.ShapeDtypeStruct((64, LANES), f32),
            jax.ShapeDtypeStruct((1,), f32),
        ),
        in_specs=[in_vmem, in_vmem],
        out_specs=(anywhere,) * 4,
        scratch_shapes=[
            flat,
            pltpu.VMEM((512, LANES), f32),
            pltpu.VMEM((24, 4, 8, LANES), f32),
            pltpu.VMEM((256, LANES), f32),
            pltpu.VMEM((64, LANES), f32),
            pltpu.SMEM((1,), f32),
            dma((5,)),
        ],
        compiler_params=pltpu.CompilerParams(vmem_limit_bytes=16 * 1024 * 1024),
    )(lines, most)
    return (block_of(cost, 32), block_of(one, 16), block_of(two, 8), change)


def solution(mesh):
    slabs = mesh.shape["rows"]
    plane = PLANE if slabs >= 32 else (2, 2)
    return jax.shard_map(
        functools.partial(shards, slabs // (plane[0] * plane[1]), plane),
        mesh=mesh,
        in_specs=(P("rows", "cols"), P("rows", "cols")),
        out_specs=(P("rows", "cols"), P("rows", "cols"), P("rows", "cols"), P()),
        check_vma=False,
    )
```

```python
import functools

import jax
import jax.numpy as jnp
from jax import lax
from jax.experimental import pallas as pl
from jax.experimental.pallas import tpu as pltpu
from jax.sharding import PartitionSpec as P

HUGE = 1e30
MESH = pl.DeviceIdType.MESH
ROWS = 32
CHUNKS = 32
LANES = 128
PLANE = (4, 4)
HUB = 1
PARTS = 4
STEPS = LANES // PARTS


def far_first(sizes):
    offsets = [()]
    for size in sizes:
        offsets = [(*o, k) for o in offsets for k in range(size)]
    hops = lambda o: sum(min(k, s - k) for k, s in zip(o, sizes))
    return sorted((o for o in offsets if any(o)), key=hops, reverse=True)


def kernel(
    nz, plane, f_hbm, s_hbm, lines_ref, most_ref,
    fn, sn, h_ref, x_ref, d_ref, u_ref, ht, xt, vf, vb, edge,
    s1a, r1a, s1b, r1b, s1c, r1c, s2a, r2a, s2b, r2b, s2c, r2c, s3, r3, s3c, r3c, pre, enter, xs, xr, paths,
    in_sem, send1, recv1, send2, recv2, send3, recv3, sendx, recvx,
):
    px, py = plane
    np_ = px * py
    width = CHUNKS // np_
    row = lax.axis_index("rows")
    core = lax.axis_index("cols")
    z, p = lax.div(row, np_), lax.rem(row, np_)
    x, y = lax.div(p, py), lax.rem(p, py)
    other_core = 1 - core
    hub = core == HUB
    tile = (4, 8, LANES)
    part = (2, width, LANES)
    near_plane = far_first(plane)
    near_z = far_first((nz,))

    def in_copies(b):
        lines = pl.ds(pl.multiple_of(b * 256, 256), 256)
        return (
            pltpu.make_async_copy(f_hbm.at[lines], fn.at[lines], in_sem.at[0, b]),
            pltpu.make_async_copy(s_hbm.at[lines], sn.at[lines], in_sem.at[1, b]),
        )

    for b in range(4):
        for copy in in_copies(b):
            copy.start()

    x_at = [x] + [lax.rem(x + d, px) for d in range(1, px)]
    y_at = [y] + [lax.rem(y + d, py) for d in range(1, py)]
    z_at = [z] + [lax.rem(z + d, nz) for d in range(1, nz)]

    def slot(k):
        dx, dy = near_plane[k]
        return x_at[dx] * py + y_at[dy]

    def z_slot(k):
        return z_at[near_z[k][0]]

    barrier = pltpu.get_barrier_semaphore()

    def greet(device):
        pl.semaphore_signal(barrier, inc=1, device_id=device, device_id_type=MESH)

    @pl.when(hub)
    def _():
        for k in range(np_ - 1):
            greet((z * np_ + slot(k), HUB))
            if k < nz - 1:
                greet((z_slot(k) * np_ + p, HUB))
            greet((z * np_ + slot(k), 1 - HUB))
        greet((row, 1 - HUB))

    def wait_for_peers():
        @pl.when(hub)
        def _():
            pl.semaphore_wait(barrier, np_ - 1 + nz - 1)

        @pl.when(jnp.logical_not(hub))
        def _():
            pl.semaphore_wait(barrier, np_)

    huge = jnp.full(tile, HUGE, jnp.float32)
    zero = jnp.zeros(tile, jnp.float32)

    def spread(b, _):
        for copy in in_copies(b):
            copy.wait()
        for s in range(8):
            for g in range(4):
                lines = pl.ds((b * 32 + g * 8) * 8 + s, 8, stride=8)
                h_ref[b * 8 + s, g] = 0.5 * fn[lines, :]
                x_ref[b * 8 + s, g] = jnp.where(sn[lines, :] == 1, 0.0, HUGE)
        return 0

    lax.fori_loop(0, ROWS // 8, spread, 0)

    def border_costs(b, carry):
        down, up, hd, hu = carry
        for s in range(8):
            i = b * 8 + s
            h = h_ref[i]
            down = jnp.minimum(x_ref[i], down + (hd + h))
            hd = h
            h = h_ref[ROWS - 1 - i]
            up = jnp.minimum(x_ref[ROWS - 1 - i], up + (hu + h))
            hu = h
        return (down, up, hd, hu)

    def add_rows(b, total):
        return sum((h_ref[b * 8 + s] for s in range(8)), start=total)

    def second_local(b, carry):
        down, up, hd, hu, far_d, far_u, most = carry
        for s in range(8):
            i = b * 8 + s
            h, v = h_ref[i], x_ref[i]
            down = jnp.minimum(v, down + (hd + h))
            far_d = jnp.maximum(v, far_d - (hd + h))
            most = jnp.maximum(most, v - down)
            hd = h
            h, v = h_ref[ROWS - 1 - i], x_ref[ROWS - 1 - i]
            up = jnp.minimum(v, up + (hu + h))
            far_u = jnp.maximum(v, far_u - (hu + h))
            most = jnp.maximum(most, v - up)
            hu = h
        return (down, up, hd, hu, far_d, far_u, most)

    def put(to, item, value):
        for q in range(np_):
            line = q * width
            to[q, item] = value[line // 8, line % 8 : line % 8 + width, :]

    def remote(src, dst, send, recv, device):
        return pltpu.make_async_remote_copy(
            src_ref=src, dst_ref=dst, send_sem=send, recv_sem=recv,
            device_id=device, device_id_type=MESH,
        )

    my_z = jnp.full(part, z, jnp.int32)
    last = np_ - 1
    not_hub = jnp.logical_not(hub)

    def to_hub(to, got, n, k):
        q = p if k == last else slot(k)
        return remote(
            to.at[q], got.at[core, p], send1.at[n, k], recv1.at[n, core, k], (z * np_ + q, HUB)
        )

    def send_to_hubs(to, got, n):
        for k in range(last):
            to_hub(to, got, n, k).start()

        @pl.when(not_hub)
        def _():
            to_hub(to, got, n, last).start()

    def sent_to_hubs(to, got, n):
        for k in range(last):
            to_hub(to, got, n, k).wait_send()

        @pl.when(not_hub)
        def _():
            to_hub(to, got, n, last).wait_send()

    def hub_has(to, got, n):
        for item in range(to.shape[1]):
            got[HUB, p, item] = to[p, item]
        for k in range(np_ - 1, -1, -1):
            for half in range(2):
                if k == last and half == HUB:
                    continue
                remote(
                    to.at[p], got.at[half, p], send1.at[n, k], recv1.at[n, half, k], (row, HUB)
                ).wait_recv()

    def along_z(source, got, n, k):
        return remote(
            source(k), got.at[z], send2.at[n, k], recv2.at[n, k], (z_slot(k) * np_ + p, HUB)
        )

    def by_side(to):
        return lambda k: to.at[lax.div(z_slot(k) - z + nz, nz)]

    def from_hub(source, got, n, half, k):
        q = p if k == last else slot(k)
        return remote(
            source(half, q), got.at[p], send3.at[n, half, k], recv3.at[n, k], (z * np_ + q, half)
        )

    to_cores = [(half, k) for half in (1 - HUB, HUB) for k in range(np_) if (half, k) != (HUB, last)]

    def cores_have(got, n):
        def copy(k):
            return remote(got.at[p], got.at[p], send3.at[n, HUB, k], recv3.at[n, k], (row, HUB))

        @pl.when(not_hub)
        def _():
            copy(last).wait_recv()

        for k in range(last - 1, -1, -1):
            copy(k).wait_recv()

    def plain(ref):
        return lambda *_: ref

    near = jnp.full(part, HUGE, jnp.float32)
    none = jnp.zeros(part, jnp.float32)
    rounds = ((s1a, r1a, s2a, r2a), (s1b, r1b, s2b, r2b))

    def vertical(step, window):
        s1, r1, s2, r2 = rounds[step]
        down, up, hd, hu = lax.fori_loop(0, ROWS // 8, border_costs, (huge, huge, zero, zero))
        put(s1, 0, up + hu)
        put(s1, 1, down + hd)
        if step == 0:
            put(s1, 2, 2.0 * lax.fori_loop(0, ROWS // 8, add_rows, zero))
            wait_for_peers()
        send_to_hubs(s1, r1, step)
        window()
        to, got = s3.at[step], r3.at[step]

        @pl.when(hub)
        def _():
            hub_has(s1, r1, step)
            b, a, s_down, s_up = near, near, none, none
            for q in range(np_):
                s = r1a[:, q, 2]
                if step == 0:
                    pre[q, 2] = s_down
                    s_down = s_down + s
                pre[q, 0] = b
                b = jnp.minimum(r1[:, q, 1], b + s)
            for q in range(np_ - 1, -1, -1):
                s = r1a[:, q, 2]
                if step == 0:
                    pre[q, 3] = s_up
                    s_up = s_up + s
                pre[q, 1] = a
                a = jnp.minimum(r1[:, q, 0], a + s)
            for side, value in enumerate((a, b)):
                s2[side, 0] = value
                if step == 0:
                    s2[side, 1] = s_down
            for k in range(nz - 1):
                along_z(by_side(s2), r2, step, k).start()
            r2[z, 0] = b
            if step == 0:
                r2[z, 1] = s_down
            else:
                hub_has(s1c, r1c, 2)
                b, far_d, far_u, most = near, -near, -near, none
                for q in range(np_):
                    s, r_p = r1a[:, q, 2], r1c[:, q, 0]
                    most = jnp.maximum(most, jnp.maximum(far_d - r1[:, q, 0], r_p - b))
                    most = jnp.maximum(most, r1c[:, q, 2])
                    far_d = jnp.maximum(r1c[:, q, 1], far_d - s)
                    b = jnp.minimum(r1[:, q, 1], b + s)
                for q in range(np_ - 1, -1, -1):
                    far_u = jnp.maximum(r1c[:, q, 0], far_u - r1a[:, q, 2])
                for item, value in enumerate((a, b, far_u, far_d, most)):
                    s2c[item] = value
                    r2c[z, item] = value
                for k in range(nz - 1):
                    along_z(plain(s2c), r2c, 2, k).start()
            for k in range(nz - 2, -1, -1):
                along_z(by_side(s2), r2, step, k).wait_recv()
            in_d, in_u = near, near
            for k in range(nz):
                in_d = jnp.where(my_z > k, jnp.minimum(r2[k, 0], in_d + r2a[k, 1]), in_d)
            for k in range(nz - 1, -1, -1):
                in_u = jnp.where(my_z < k, jnp.minimum(r2[k, 0], in_u + r2a[k, 1]), in_u)
            for q in range(np_):
                to[:, q, 0] = jnp.minimum(pre[q, 0], in_d + pre[q, 2])
                to[:, q, 1] = jnp.minimum(pre[q, 1], in_u + pre[q, 3])
            for half, k in to_cores:
                from_hub(lambda h, q: to.at[h, q], got, step, half, k).start()
            for item in range(2):
                got[p, item] = to[HUB, p, item]
            if step == 1:
                for k in range(nz - 2, -1, -1):
                    along_z(plain(s2c), r2c, 2, k).wait_recv()
                b, far_d, most = near, -near, none
                for k in range(nz):
                    s = r2a[k, 1]
                    most = jnp.maximum(most, jnp.maximum(far_d - r2c[k, 0], r2c[k, 2] - b))
                    most = jnp.maximum(most, r2c[k, 4])
                    far_d = jnp.maximum(r2c[k, 3], far_d - s)
                    b = jnp.minimum(r2c[k, 1], b + s)
                most = jnp.maximum(most[0], most[1])
                s3c[...] = most
                r3c[p] = most
                for half, k in to_cores:
                    from_hub(plain(s3c), r3c, 2, half, k).start()

        cores_have(got, step)
        for q in range(np_):
            line = q * width
            for item in range(2):
                enter[item, line // 8, line % 8 : line % 8 + width, :] = got[q, item]

        def final(b, carry):
            down, up, hd, hu = carry
            for s in range(8):
                i = b * 8 + s
                h = h_ref[i]
                down = jnp.minimum(x_ref[i], down + (hd + h))
                d_ref[i] = down
                hd = h
                h = h_ref[ROWS - 1 - i]
                up = jnp.minimum(x_ref[ROWS - 1 - i], up + (hu + h))
                u_ref[ROWS - 1 - i] = up
                hu = h
            return (down, up, hd, hu)

        lax.fori_loop(0, ROWS // 8, final, (enter[0], enter[1], zero, zero))

    def second_window():
        _, _, hd, hu, far_d, far_u, most = lax.fori_loop(
            0, ROWS // 8, second_local, (huge, huge, zero, zero, -huge, -huge, zero)
        )
        put(s1c, 0, far_u - hu)
        put(s1c, 1, far_d - hd)
        put(s1c, 2, most)
        send_to_hubs(s1c, r1c, 2)

    def drain(step):
        s1, r1, s2, r2 = rounds[step]
        sent_to_hubs(s1, r1, step)
        to, got = s3.at[step], r3.at[step]
        if step == 1:
            sent_to_hubs(s1c, r1c, 2)
            cores_have(r3c, 2)

        @pl.when(hub)
        def _():
            for k in range(nz - 1):
                along_z(by_side(s2), r2, step, k).wait_send()
                if step == 1:
                    along_z(plain(s2c), r2c, 2, k).wait_send()
            for half, k in to_cores:
                from_hub(lambda h, q: to.at[h, q], got, step, half, k).wait_send()
                if step == 1:
                    from_hub(plain(s3c), r3c, 2, half, k).wait_send()

    lane = lax.broadcasted_iota(jnp.int32, (8, LANES), 1)
    sub = lax.broadcasted_iota(jnp.int32, (8, LANES), 0)
    inner, outer = lane % 8, sub % 4
    huge2 = jnp.full((8, LANES), HUGE, jnp.float32)
    zero2 = jnp.zeros((8, LANES), jnp.float32)

    def block(load, j):
        return load(pl.ds((j // 4) * 16, 16), j % 4).reshape(LANES, LANES)

    def at(i):
        return pl.ds(pl.multiple_of(i * 8, 8), 8)

    def chunk_path(shift):
        return paths[11 + shift]

    def group_path(shift):
        return paths[22 + shift]

    def measure():
        for j in range(8):
            ht[pl.ds(j, LANES, stride=8), :] = block(lambda r, g: h_ref[r, g], j).T

        def add(b, sums):
            return tuple(
                sum((ht[at(k * STEPS + b * 8 + s), :] for s in range(8)), start=sums[k])
                for k in range(PARTS)
            )

        sums = lax.fori_loop(0, STEPS // 8, add, (zero2,) * PARTS)
        for k in range(PARTS):
            paths[k] = 2.0 * sums[k]
        whole = 2.0 * (sums[0] + sums[1] + sums[2] + sums[3])
        before = after = zero2
        for k in range(-7, 8):
            rolled = pltpu.roll(whole, k % LANES, 1)
            paths[11 + k] = rolled
            if k > 0:
                before = jnp.where(inner >= k, before + rolled, before)
            if k < 0:
                after = jnp.where(inner - k < 8, after + rolled, after)
        paths[26] = before
        paths[27] = after
        whole = before + whole + after
        before = after = zero2
        for k in range(-3, 4):
            rolled = pltpu.roll(whole, k % 8, 0)
            paths[22 + k] = rolled
            if k > 0:
                before = jnp.where(outer >= k, before + rolled, before)
            if k < 0:
                after = jnp.where(outer - k < 4, after + rolled, after)
        paths[28] = before
        paths[29] = after

        def border(b, path):
            for t in range(8):
                i = b * 8 + t
                i = core * i + other_core * (LANES - 1 - i)
                h = ht[at(i), :]
                edge[at(i), :] = path + h
                path = path + 2.0 * h
            return path

        first = jnp.full((8, LANES), core, jnp.int32) == 0
        lax.fori_loop(
            0, LANES // 8, border, jnp.where(first, paths[27] + paths[29], paths[26] + paths[28])
        )

    def scan_all(c, path, axis, size, place, forward):
        step = 1 if forward else -1
        extent = c.shape[axis]
        at_place = place if forward else size - 1 - place
        run = huge2
        for k in range(size - 1, 0, -1):
            ck = pltpu.roll(c, (step * k) % extent, axis)
            run = jnp.where(at_place >= k, jnp.minimum(ck, run + path(step * k)), run)
        before = run
        run = jnp.minimum(c, run + path(0))
        for k in range(1, size):
            ck = pltpu.roll(c, (-step * k) % extent, axis)
            run = jnp.where(at_place + k < size, jnp.minimum(ck, run + path(-step * k)), run)
        return before, run

    def horizontal(step, window):
        for j in range(8):
            rows = pl.ds(j, LANES, stride=8)
            xt[rows, :] = block(lambda r, g: jnp.minimum(d_ref[r, g], u_ref[r, g]), j).T

        def sweep(start_f, start_b, store):
            def some(b, carry):
                right, left, hr, hl = (list(c) for c in carry)
                for s in range(8):
                    for k in range(PARTS):
                        i = k * STEPS + b * 8 + s
                        h = ht[at(i), :]
                        right[k] = jnp.minimum(xt[at(i), :], right[k] + (hr[k] + h))
                        if store:
                            vf[at(i), :] = right[k]
                        hr[k] = h
                        i = (k + 1) * STEPS - 1 - (b * 8 + s)
                        h = ht[at(i), :]
                        left[k] = jnp.minimum(xt[at(i), :], left[k] + (hl[k] + h))
                        if store:
                            vb[at(i), :] = left[k]
                        hl[k] = h
                return (tuple(right), tuple(left), tuple(hr), tuple(hl))

            zeros = (zero2,) * PARTS
            return lax.fori_loop(0, STEPS // 8, some, (start_f, start_b, zeros, zeros))

        right, left, hr, hl = sweep((huge2,) * PARTS, (huge2,) * PARTS, False)
        right = [r + h for r, h in zip(right, hr)]
        left = [r + h for r, h in zip(left, hl)]
        c_f, c_b = right[0], left[-1]
        for k in range(1, PARTS):
            c_f = jnp.minimum(right[k], c_f + paths[k])
            c_b = jnp.minimum(left[-1 - k], c_b + paths[PARTS - 1 - k])
        fc, f_all = scan_all(c_f, chunk_path, 1, 8, inner, True)
        bc, b_all = scan_all(c_b, chunk_path, 1, 8, inner, False)
        gfc, gf_all = scan_all(f_all, group_path, 0, 4, outer, True)
        gbc, gb_all = scan_all(b_all, group_path, 0, 4, outer, False)
        first = jnp.full((8, LANES), core, jnp.int32) == 0
        xs[step] = jnp.where(first, gf_all, gb_all)
        copy = remote(xs.at[step], xr.at[step], sendx.at[step], recvx.at[step], (row, other_core))
        copy.start()
        in_f = [jnp.minimum(fc, gfc + paths[26])]
        in_b = [jnp.minimum(bc, gbc + paths[27])]
        for k in range(PARTS - 1):
            in_f.append(jnp.minimum(right[k], in_f[k] + paths[k]))
            in_b.append(jnp.minimum(left[-1 - k], in_b[k] + paths[PARTS - 1 - k]))
        sweep(tuple(in_f), tuple(in_b[::-1]), True)
        window()
        copy.wait()
        return xr[step]

    def in_row(other, j):
        rows = pl.ds(j, LANES, stride=8)
        return jnp.minimum(jnp.minimum(vf[rows, :], vb[rows, :]), edge[rows, :] + other[j : j + 1])

    vertical(0, measure)
    other = horizontal(0, lambda: drain(0))
    for j in range(8):
        back = in_row(other, j).T
        x_ref[pl.ds((j // 4) * 16, 16), j % 4] = back.reshape(16, 8, LANES)
    vertical(1, second_window)
    other = horizontal(1, lambda: drain(1))
    most = r3c[0]
    for q in range(1, np_):
        most = jnp.maximum(most, r3c[q])
    most_ref[...] = most

    def merge(b, _):
        for t in range(16):
            i = at(b * 16 + t)
            lines_ref[i, :] = jnp.minimum(jnp.minimum(vf[i, :], vb[i, :]), edge[i, :] + other)
        return 0

    lax.fori_loop(0, 8, merge, 0)


def finish(xt, most, cost_hbm, one_hbm, two_hbm, change_hbm, on, pairs, pool, o1, o2, change, out_sem):
    lane = lax.broadcasted_iota(jnp.int32, (8, LANES), 1)
    change[0] = jnp.max(most[...])
    outs = [pltpu.make_async_copy(change, change_hbm, out_sem.at[4])]
    outs[0].start()
    for j in range(8):
        back = xt[pl.ds(j, LANES, stride=8), :].T
        for r in range(16):
            i = (j // 4) * 16 + r
            lines = pl.ds(((i // 8) * 32 + (j % 4) * 8) * 8 + i % 8, 8, stride=8)
            on[lines, :] = back[r * 8 : (r + 1) * 8, :]
        if j % 4 == 3:
            half = pl.ds((j // 4) * 512, 512)
            outs.append(pltpu.make_async_copy(on.at[half], cost_hbm.at[half], out_sem.at[2 + j // 4]))
            outs[-1].start()

    for j in range(8):
        pair = jnp.minimum(xt[pl.ds(j, 64, stride=16), :], xt[pl.ds(j + 8, 64, stride=16), :])
        lines = jnp.concatenate([pair, pair], axis=0).T.reshape(8, 2, 8, LANES)
        pool[pl.ds((j // 4) * 8, 8), j % 4] = jnp.minimum(lines[:, 0], lines[:, 1])
        pairs[pl.ds(j, 64, stride=8), :] = pair
    for a in range(16):
        for g in range(2):
            halves = [
                jnp.concatenate([pool[a, 2 * g + t, pl.ds(i, 4, stride=2), :] for t in range(2)], axis=0)
                for i in range(2)
            ]
            lines = pl.ds(((a // 8) * 16 + g * 8) * 8 + a % 8, 8, stride=8)
            o1[lines, :] = jnp.where(lane < 64, halves[0], halves[1])
    out_one = pltpu.make_async_copy(o1, one_hbm, out_sem.at[0])
    out_one.start()

    for j in range(8):
        quad = jnp.minimum(pairs[pl.ds(j, 32, stride=16), :], pairs[pl.ds(j + 8, 32, stride=16), :])
        lines = jnp.concatenate([quad] * 4, axis=0).T.reshape(4, 4, 8, LANES)
        lines = jnp.minimum(
            jnp.minimum(lines[:, 0], lines[:, 1]), jnp.minimum(lines[:, 2], lines[:, 3])
        )
        pool[pl.ds(16 + (j // 4) * 4, 4), j % 4] = lines
    for a in range(8):
        quarters = [
            jnp.concatenate([pool[16 + a, g, pl.ds(i, 2, stride=4), :] for g in range(4)], axis=0)
            for i in range(4)
        ]
        low = jnp.where(lane < 32, quarters[0], quarters[1])
        high = jnp.where(lane < 96, quarters[2], quarters[3])
        o2[pl.ds(a, 8, stride=8), :] = jnp.where(lane < 64, low, high)
    out_two = pltpu.make_async_copy(o2, two_hbm, out_sem.at[1])
    out_two.start()
    for out in outs:
        out.wait()
    out_one.wait()
    out_two.wait()


def lines_of(block):
    height, length = block.shape
    return (
        block.reshape(height // 8, 8, length // LANES, LANES)
        .transpose(0, 2, 1, 3)
        .reshape(-1, LANES)
    )


def block_of(lines, height):
    return lines.reshape(height // 8, -1, 8, LANES).transpose(0, 2, 1, 3).reshape(height, -1)


def shards(nz, plane, friction, sources):
    np_ = plane[0] * plane[1]
    width = CHUNKS // np_
    f32 = jnp.float32
    anywhere = pl.BlockSpec(memory_space=pltpu.HBM)
    in_vmem = pl.BlockSpec(memory_space=pltpu.VMEM)
    field = pltpu.VMEM((ROWS, 4, 8, LANES), f32)
    flat = pltpu.VMEM((ROWS * CHUNKS, LANES), f32)
    dma = pltpu.SemaphoreType.DMA

    def message(count, items, *halves):
        return pltpu.VMEM((*count, items, *halves, width, LANES), f32)

    def in_hbm(block):
        return pltpu.with_memory_space_constraint(lines_of(block), pltpu.HBM)

    rounds = []
    for items in (3, 2, 3):
        rounds += [message((np_,), items), message((2, np_), items)]
    for sides, items in (((2,), 2), ((2,), 1), ((), 5)):
        rounds += [message(sides, items, 2), message((nz,), items, 2)]
    lines, most = pl.pallas_call(
        functools.partial(kernel, nz, plane),
        out_shape=(jax.ShapeDtypeStruct((1024, LANES), f32), jax.ShapeDtypeStruct((width, LANES), f32)),
        in_specs=[anywhere, anywhere],
        out_specs=(in_vmem, in_vmem),
        scratch_shapes=[
            flat,
            pltpu.VMEM((ROWS * CHUNKS, LANES), jnp.int32),
            field, field, field, field,
            flat, flat, flat, flat, flat,
            *rounds,
            message((2, 2, np_), 2),
            message((2, np_), 2),
            pltpu.VMEM((width, LANES), f32),
            pltpu.VMEM((np_, width, LANES), f32),
            message((np_,), 4, 2),
            pltpu.VMEM((2, 4, 8, LANES), f32),
            pltpu.VMEM((2, 8, LANES), f32),
            pltpu.VMEM((2, 8, LANES), f32),
            pltpu.VMEM((30, 8, LANES), f32),
            dma((2, 4)),
            dma((3, np_)), dma((3, 2, np_)),
            dma((3, nz)), dma((3, nz)),
            dma((3, 2, np_)), dma((3, np_)),
            dma((2,)), dma((2,)),
        ],
        compiler_params=pltpu.CompilerParams(
            collective_id=0, has_side_effects=True, vmem_limit_bytes=16 * 1024 * 1024
        ),
    )(in_hbm(friction), in_hbm(sources))
    cost, one, two, change = pl.pallas_call(
        finish,
        out_shape=(
            jax.ShapeDtypeStruct((1024, LANES), f32),
            jax.ShapeDtypeStruct((256, LANES), f32),
            jax.ShapeDtypeStruct((64, LANES), f32),
            jax.ShapeDtypeStruct((1,), f32),
        ),
        in_specs=[in_vmem, in_vmem],
        out_specs=(anywhere,) * 4,
        scratch_shapes=[
            flat,
            pltpu.VMEM((512, LANES), f32),
            pltpu.VMEM((24, 4, 8, LANES), f32),
            pltpu.VMEM((256, LANES), f32),
            pltpu.VMEM((64, LANES), f32),
            pltpu.SMEM((1,), f32),
            dma((5,)),
        ],
        compiler_params=pltpu.CompilerParams(vmem_limit_bytes=16 * 1024 * 1024),
    )(lines, most)
    return (block_of(cost, 32), block_of(one, 16), block_of(two, 8), change)


def solution(mesh):
    slabs = mesh.shape["rows"]
    plane = PLANE if slabs >= 32 else (2, 2)
    return jax.shard_map(
        functools.partial(shards, slabs // (plane[0] * plane[1]), plane),
        mesh=mesh,
        in_specs=(P("rows", "cols"), P("rows", "cols")),
        out_specs=(P("rows", "cols"), P("rows", "cols"), P("rows", "cols"), P()),
        check_vma=False,
    )
```

```python
import functools

import jax
import jax.numpy as jnp
from jax import lax
from jax.experimental import pallas as pl
from jax.experimental.pallas import tpu as pltpu
from jax.sharding import PartitionSpec as P

HUGE = 1e30
MESH = pl.DeviceIdType.MESH
ROWS = 32
CHUNKS = 32
LANES = 128
PLANE = (4, 4)
HUB = 1
PARTS = 4
STEPS = LANES // PARTS


def far_first(sizes):
    offsets = [()]
    for size in sizes:
        offsets = [(*o, k) for o in offsets for k in range(size)]
    hops = lambda o: sum(min(k, s - k) for k, s in zip(o, sizes))
    return sorted((o for o in offsets if any(o)), key=hops, reverse=True)


def kernel(
    nz, plane, f_hbm, s_hbm, lines_ref, most_ref,
    fn, sn, h_ref, x_ref, d_ref, u_ref, ht, xt, vf, vb, edge,
    s1a, r1a, s1b, r1b, s1c, r1c, s2a, r2a, s2b, r2b, s2c, r2c, s3, r3, s3c, r3c, pre, enter, xs, xr, paths,
    in_sem, send1, recv1, send2, recv2, send3, recv3, sendx, recvx,
):
    px, py = plane
    np_ = px * py
    width = CHUNKS // np_
    row = lax.axis_index("rows")
    core = lax.axis_index("cols")
    z, p = lax.div(row, np_), lax.rem(row, np_)
    x, y = lax.div(p, py), lax.rem(p, py)
    other_core = 1 - core
    hub = core == HUB
    tile = (4, 8, LANES)
    part = (2, width, LANES)
    near_plane = far_first(plane)
    near_z = far_first((nz,))

    loads = (
        pltpu.make_async_copy(f_hbm, fn, in_sem.at[0]),
        pltpu.make_async_copy(s_hbm, sn, in_sem.at[1]),
    )
    for load in loads:
        load.start()

    x_at = [x] + [lax.rem(x + d, px) for d in range(1, px)]
    y_at = [y] + [lax.rem(y + d, py) for d in range(1, py)]
    z_at = [z] + [lax.rem(z + d, nz) for d in range(1, nz)]

    def slot(k):
        dx, dy = near_plane[k]
        return x_at[dx] * py + y_at[dy]

    def z_slot(k):
        return z_at[near_z[k][0]]

    barrier = pltpu.get_barrier_semaphore()

    def greet(device):
        pl.semaphore_signal(barrier, inc=1, device_id=device, device_id_type=MESH)

    @pl.when(hub)
    def _():
        for k in range(np_ - 1):
            greet((z * np_ + slot(k), HUB))
            if k < nz - 1:
                greet((z_slot(k) * np_ + p, HUB))
            greet((z * np_ + slot(k), 1 - HUB))
        greet((row, 1 - HUB))

    def wait_for_peers():
        @pl.when(hub)
        def _():
            pl.semaphore_wait(barrier, np_ - 1 + nz - 1)

        @pl.when(jnp.logical_not(hub))
        def _():
            pl.semaphore_wait(barrier, np_)

    huge = jnp.full(tile, HUGE, jnp.float32)
    zero = jnp.zeros(tile, jnp.float32)

    def spread(b, _):
        for s in range(8):
            for g in range(4):
                lines = pl.ds((b * 32 + g * 8) * 8 + s, 8, stride=8)
                h_ref[b * 8 + s, g] = 0.5 * fn[lines, :]
                x_ref[b * 8 + s, g] = jnp.where(sn[lines, :] == 1, 0.0, HUGE)
        return 0

    for load in loads:
        load.wait()
    lax.fori_loop(0, ROWS // 8, spread, 0)

    def border_costs(b, carry):
        down, up, hd, hu = carry
        for s in range(8):
            i = b * 8 + s
            h = h_ref[i]
            down = jnp.minimum(x_ref[i], down + (hd + h))
            hd = h
            h = h_ref[ROWS - 1 - i]
            up = jnp.minimum(x_ref[ROWS - 1 - i], up + (hu + h))
            hu = h
        return (down, up, hd, hu)

    def add_rows(b, total):
        return sum((h_ref[b * 8 + s] for s in range(8)), start=total)

    def second_local(b, carry):
        down, up, hd, hu, far_d, far_u, most = carry
        for s in range(8):
            i = b * 8 + s
            h, v = h_ref[i], x_ref[i]
            down = jnp.minimum(v, down + (hd + h))
            far_d = jnp.maximum(v, far_d - (hd + h))
            most = jnp.maximum(most, v - down)
            hd = h
            h, v = h_ref[ROWS - 1 - i], x_ref[ROWS - 1 - i]
            up = jnp.minimum(v, up + (hu + h))
            far_u = jnp.maximum(v, far_u - (hu + h))
            most = jnp.maximum(most, v - up)
            hu = h
        return (down, up, hd, hu, far_d, far_u, most)

    def put(to, item, value):
        for q in range(np_):
            line = q * width
            to[q, item] = value[line // 8, line % 8 : line % 8 + width, :]

    def remote(src, dst, send, recv, device):
        return pltpu.make_async_remote_copy(
            src_ref=src, dst_ref=dst, send_sem=send, recv_sem=recv,
            device_id=device, device_id_type=MESH,
        )

    my_z = jnp.full(part, z, jnp.int32)
    last = np_ - 1
    not_hub = jnp.logical_not(hub)

    def to_hub(to, got, n, k):
        q = p if k == last else slot(k)
        return remote(
            to.at[q], got.at[core, p], send1.at[n], recv1.at[n, core], (z * np_ + q, HUB)
        )

    def send_to_hubs(to, got, n):
        for k in range(last):
            to_hub(to, got, n, k).start()

        @pl.when(not_hub)
        def _():
            to_hub(to, got, n, last).start()

    def arrived(ref, sem):
        remote(ref, ref, send1.at[0], sem, (row, HUB)).wait_recv()

    def sent(ref, sem):
        remote(ref, ref, sem, recv1.at[0, 0], (row, HUB)).wait_send()

    def sent_to_hubs(to, got, n):
        @pl.when(hub)
        def _():
            sent(to.at[pl.ds(0, last)], send1.at[n])

        @pl.when(not_hub)
        def _():
            sent(to, send1.at[n])

    def hub_has(to, got, n):
        for item in range(to.shape[1]):
            got[HUB, p, item] = to[p, item]
        arrived(got.at[HUB, pl.ds(0, last)], recv1.at[n, HUB])
        arrived(got.at[1 - HUB], recv1.at[n, 1 - HUB])

    def along_z(source, got, n, k):
        return remote(
            source(k), got.at[z], send2.at[n], recv2.at[n], (z_slot(k) * np_ + p, HUB)
        )

    def by_side(to):
        return lambda k: to.at[lax.div(z_slot(k) - z + nz, nz)]

    def from_hub(source, got, n, half, k):
        q = p if k == last else slot(k)
        return remote(
            source(half, q), got.at[p], send3.at[n, half], recv3.at[n], (z * np_ + q, half)
        )

    to_cores = [(half, k) for half in (1 - HUB, HUB) for k in range(np_) if (half, k) != (HUB, last)]

    def cores_have(got, n):
        @pl.when(hub)
        def _():
            arrived(got.at[pl.ds(0, last)], recv3.at[n])

        @pl.when(not_hub)
        def _():
            arrived(got, recv3.at[n])

    def sent_to_cores(got, n):
        sent(got, send3.at[n, 1 - HUB])
        sent(got.at[pl.ds(0, last)], send3.at[n, HUB])

    def plain(ref):
        return lambda *_: ref

    near = jnp.full(part, HUGE, jnp.float32)
    none = jnp.zeros(part, jnp.float32)
    rounds = ((s1a, r1a, s2a, r2a), (s1b, r1b, s2b, r2b))

    def vertical(step, window):
        s1, r1, s2, r2 = rounds[step]
        down, up, hd, hu = lax.fori_loop(0, ROWS // 8, border_costs, (huge, huge, zero, zero))
        put(s1, 0, up + hu)
        put(s1, 1, down + hd)
        if step == 0:
            put(s1, 2, 2.0 * lax.fori_loop(0, ROWS // 8, add_rows, zero))
            wait_for_peers()
        send_to_hubs(s1, r1, step)
        window()
        to, got = s3.at[step], r3.at[step]

        @pl.when(hub)
        def _():
            hub_has(s1, r1, step)
            b, a, s_down, s_up = near, near, none, none
            for q in range(np_):
                s = r1a[:, q, 2]
                if step == 0:
                    pre[q, 2] = s_down
                    s_down = s_down + s
                pre[q, 0] = b
                b = jnp.minimum(r1[:, q, 1], b + s)
            for q in range(np_ - 1, -1, -1):
                s = r1a[:, q, 2]
                if step == 0:
                    pre[q, 3] = s_up
                    s_up = s_up + s
                pre[q, 1] = a
                a = jnp.minimum(r1[:, q, 0], a + s)
            for side, value in enumerate((a, b)):
                s2[side, 0] = value
                if step == 0:
                    s2[side, 1] = s_down
            for k in range(nz - 1):
                along_z(by_side(s2), r2, step, k).start()
            r2[z, 0] = b
            if step == 0:
                r2[z, 1] = s_down
            else:
                hub_has(s1c, r1c, 2)
                b, far_d, far_u, most = near, -near, -near, none
                for q in range(np_):
                    s, r_p = r1a[:, q, 2], r1c[:, q, 0]
                    most = jnp.maximum(most, jnp.maximum(far_d - r1[:, q, 0], r_p - b))
                    most = jnp.maximum(most, r1c[:, q, 2])
                    far_d = jnp.maximum(r1c[:, q, 1], far_d - s)
                    b = jnp.minimum(r1[:, q, 1], b + s)
                for q in range(np_ - 1, -1, -1):
                    far_u = jnp.maximum(r1c[:, q, 0], far_u - r1a[:, q, 2])
                for item, value in enumerate((a, b, far_u, far_d, most)):
                    s2c[item] = value
                    r2c[z, item] = value
                for k in range(nz - 1):
                    along_z(plain(s2c), r2c, 2, k).start()
            arrived(r2.at[pl.ds(0, nz - 1)], recv2.at[step])
            in_d, in_u = near, near
            for k in range(nz):
                in_d = jnp.where(my_z > k, jnp.minimum(r2[k, 0], in_d + r2a[k, 1]), in_d)
            for k in range(nz - 1, -1, -1):
                in_u = jnp.where(my_z < k, jnp.minimum(r2[k, 0], in_u + r2a[k, 1]), in_u)
            for q in range(np_):
                to[:, q, 0] = jnp.minimum(pre[q, 0], in_d + pre[q, 2])
                to[:, q, 1] = jnp.minimum(pre[q, 1], in_u + pre[q, 3])
            for half, k in to_cores:
                from_hub(lambda h, q: to.at[h, q], got, step, half, k).start()
            for item in range(2):
                got[p, item] = to[HUB, p, item]
            if step == 1:
                arrived(r2c.at[pl.ds(0, nz - 1)], recv2.at[2])
                b, far_d, most = near, -near, none
                for k in range(nz):
                    s = r2a[k, 1]
                    most = jnp.maximum(most, jnp.maximum(far_d - r2c[k, 0], r2c[k, 2] - b))
                    most = jnp.maximum(most, r2c[k, 4])
                    far_d = jnp.maximum(r2c[k, 3], far_d - s)
                    b = jnp.minimum(r2c[k, 1], b + s)
                most = jnp.maximum(most[0], most[1])
                s3c[...] = most
                r3c[p] = most
                for half, k in to_cores:
                    from_hub(plain(s3c), r3c, 2, half, k).start()

        cores_have(got, step)
        for q in range(np_):
            line = q * width
            for item in range(2):
                enter[item, line // 8, line % 8 : line % 8 + width, :] = got[q, item]

        def final(b, carry):
            down, up, hd, hu = carry
            for s in range(8):
                i = b * 8 + s
                h = h_ref[i]
                down = jnp.minimum(x_ref[i], down + (hd + h))
                d_ref[i] = down
                hd = h
                h = h_ref[ROWS - 1 - i]
                up = jnp.minimum(x_ref[ROWS - 1 - i], up + (hu + h))
                u_ref[ROWS - 1 - i] = up
                hu = h
            return (down, up, hd, hu)

        lax.fori_loop(0, ROWS // 8, final, (enter[0], enter[1], zero, zero))

    def second_window():
        _, _, hd, hu, far_d, far_u, most = lax.fori_loop(
            0, ROWS // 8, second_local, (huge, huge, zero, zero, -huge, -huge, zero)
        )
        put(s1c, 0, far_u - hu)
        put(s1c, 1, far_d - hd)
        put(s1c, 2, most)
        send_to_hubs(s1c, r1c, 2)

    def drain(step):
        s1, r1, s2, r2 = rounds[step]
        sent_to_hubs(s1, r1, step)
        to, got = s3.at[step], r3.at[step]
        if step == 1:
            sent_to_hubs(s1c, r1c, 2)
            cores_have(r3c, 2)

        @pl.when(hub)
        def _():
            sent(r2.at[pl.ds(0, nz - 1)], send2.at[step])
            sent_to_cores(got, step)
            if step == 1:
                sent(r2c.at[pl.ds(0, nz - 1)], send2.at[2])
                sent_to_cores(r3c, 2)

    lane = lax.broadcasted_iota(jnp.int32, (8, LANES), 1)
    sub = lax.broadcasted_iota(jnp.int32, (8, LANES), 0)
    inner, outer = lane % 8, sub % 4
    huge2 = jnp.full((8, LANES), HUGE, jnp.float32)
    zero2 = jnp.zeros((8, LANES), jnp.float32)

    def block(load, j):
        return load(pl.ds((j // 4) * 16, 16), j % 4).reshape(LANES, LANES)

    def at(i):
        return pl.ds(pl.multiple_of(i * 8, 8), 8)

    def chunk_path(shift):
        return paths[11 + shift]

    def group_path(shift):
        return paths[22 + shift]

    def measure():
        for j in range(8):
            ht[pl.ds(j, LANES, stride=8), :] = block(lambda r, g: h_ref[r, g], j).T

        def add(b, sums):
            return tuple(
                sum((ht[at(k * STEPS + b * 8 + s), :] for s in range(8)), start=sums[k])
                for k in range(PARTS)
            )

        sums = lax.fori_loop(0, STEPS // 8, add, (zero2,) * PARTS)
        for k in range(PARTS):
            paths[k] = 2.0 * sums[k]
        whole = 2.0 * (sums[0] + sums[1] + sums[2] + sums[3])
        before = after = zero2
        for k in range(-7, 8):
            rolled = pltpu.roll(whole, k % LANES, 1)
            paths[11 + k] = rolled
            if k > 0:
                before = jnp.where(inner >= k, before + rolled, before)
            if k < 0:
                after = jnp.where(inner - k < 8, after + rolled, after)
        paths[26] = before
        paths[27] = after
        whole = before + whole + after
        before = after = zero2
        for k in range(-3, 4):
            rolled = pltpu.roll(whole, k % 8, 0)
            paths[22 + k] = rolled
            if k > 0:
                before = jnp.where(outer >= k, before + rolled, before)
            if k < 0:
                after = jnp.where(outer - k < 4, after + rolled, after)
        paths[28] = before
        paths[29] = after

        def border(b, path):
            for t in range(8):
                i = b * 8 + t
                i = core * i + other_core * (LANES - 1 - i)
                h = ht[at(i), :]
                edge[at(i), :] = path + h
                path = path + 2.0 * h
            return path

        first = jnp.full((8, LANES), core, jnp.int32) == 0
        lax.fori_loop(
            0, LANES // 8, border, jnp.where(first, paths[27] + paths[29], paths[26] + paths[28])
        )

    def scan_all(c, path, axis, size, place, forward):
        step = 1 if forward else -1
        extent = c.shape[axis]
        at_place = place if forward else size - 1 - place
        run = huge2
        for k in range(size - 1, 0, -1):
            ck = pltpu.roll(c, (step * k) % extent, axis)
            run = jnp.where(at_place >= k, jnp.minimum(ck, run + path(step * k)), run)
        before = run
        run = jnp.minimum(c, run + path(0))
        for k in range(1, size):
            ck = pltpu.roll(c, (-step * k) % extent, axis)
            run = jnp.where(at_place + k < size, jnp.minimum(ck, run + path(-step * k)), run)
        return before, run

    def horizontal(step, window):
        for j in range(8):
            rows = pl.ds(j, LANES, stride=8)
            xt[rows, :] = block(lambda r, g: jnp.minimum(d_ref[r, g], u_ref[r, g]), j).T

        def sweep(start_f, start_b, store):
            def some(b, carry):
                right, left, hr, hl = (list(c) for c in carry)
                for s in range(8):
                    for k in range(PARTS):
                        i = k * STEPS + b * 8 + s
                        h = ht[at(i), :]
                        right[k] = jnp.minimum(xt[at(i), :], right[k] + (hr[k] + h))
                        if store:
                            vf[at(i), :] = right[k]
                        hr[k] = h
                        i = (k + 1) * STEPS - 1 - (b * 8 + s)
                        h = ht[at(i), :]
                        left[k] = jnp.minimum(xt[at(i), :], left[k] + (hl[k] + h))
                        if store:
                            vb[at(i), :] = left[k]
                        hl[k] = h
                return (tuple(right), tuple(left), tuple(hr), tuple(hl))

            zeros = (zero2,) * PARTS
            return lax.fori_loop(0, STEPS // 8, some, (start_f, start_b, zeros, zeros))

        right, left, hr, hl = sweep((huge2,) * PARTS, (huge2,) * PARTS, False)
        right = [r + h for r, h in zip(right, hr)]
        left = [r + h for r, h in zip(left, hl)]
        c_f, c_b = right[0], left[-1]
        for k in range(1, PARTS):
            c_f = jnp.minimum(right[k], c_f + paths[k])
            c_b = jnp.minimum(left[-1 - k], c_b + paths[PARTS - 1 - k])
        fc, f_all = scan_all(c_f, chunk_path, 1, 8, inner, True)
        bc, b_all = scan_all(c_b, chunk_path, 1, 8, inner, False)
        gfc, gf_all = scan_all(f_all, group_path, 0, 4, outer, True)
        gbc, gb_all = scan_all(b_all, group_path, 0, 4, outer, False)
        first = jnp.full((8, LANES), core, jnp.int32) == 0
        xs[step] = jnp.where(first, gf_all, gb_all)
        copy = remote(xs.at[step], xr.at[step], sendx.at[step], recvx.at[step], (row, other_core))
        copy.start()
        in_f = [jnp.minimum(fc, gfc + paths[26])]
        in_b = [jnp.minimum(bc, gbc + paths[27])]
        for k in range(PARTS - 1):
            in_f.append(jnp.minimum(right[k], in_f[k] + paths[k]))
            in_b.append(jnp.minimum(left[-1 - k], in_b[k] + paths[PARTS - 1 - k]))
        sweep(tuple(in_f), tuple(in_b[::-1]), True)
        window()
        copy.wait()
        return xr[step]

    def in_row(other, j):
        rows = pl.ds(j, LANES, stride=8)
        return jnp.minimum(jnp.minimum(vf[rows, :], vb[rows, :]), edge[rows, :] + other[j : j + 1])

    vertical(0, measure)
    other = horizontal(0, lambda: drain(0))
    for j in range(8):
        back = in_row(other, j).T
        x_ref[pl.ds((j // 4) * 16, 16), j % 4] = back.reshape(16, 8, LANES)
    vertical(1, second_window)
    other = horizontal(1, lambda: drain(1))
    most = r3c[0]
    for q in range(1, np_):
        most = jnp.maximum(most, r3c[q])
    most_ref[...] = most

    def merge(b, _):
        for t in range(16):
            i = at(b * 16 + t)
            lines_ref[i, :] = jnp.minimum(jnp.minimum(vf[i, :], vb[i, :]), edge[i, :] + other)
        return 0

    lax.fori_loop(0, 8, merge, 0)


def finish(xt, most, cost_hbm, one_hbm, two_hbm, change_hbm, on, pairs, pool, o1, o2, change, out_sem):
    lane = lax.broadcasted_iota(jnp.int32, (8, LANES), 1)
    change[0] = jnp.max(most[...])
    outs = [pltpu.make_async_copy(change, change_hbm, out_sem.at[4])]
    outs[0].start()
    for j in range(8):
        back = xt[pl.ds(j, LANES, stride=8), :].T
        for r in range(16):
            i = (j // 4) * 16 + r
            lines = pl.ds(((i // 8) * 32 + (j % 4) * 8) * 8 + i % 8, 8, stride=8)
            on[lines, :] = back[r * 8 : (r + 1) * 8, :]
        if j % 4 == 3:
            half = pl.ds((j // 4) * 512, 512)
            outs.append(pltpu.make_async_copy(on.at[half], cost_hbm.at[half], out_sem.at[2 + j // 4]))
            outs[-1].start()

    for j in range(8):
        pair = jnp.minimum(xt[pl.ds(j, 64, stride=16), :], xt[pl.ds(j + 8, 64, stride=16), :])
        lines = jnp.concatenate([pair, pair], axis=0).T.reshape(8, 2, 8, LANES)
        pool[pl.ds((j // 4) * 8, 8), j % 4] = jnp.minimum(lines[:, 0], lines[:, 1])
        pairs[pl.ds(j, 64, stride=8), :] = pair
    for a in range(16):
        for g in range(2):
            halves = [
                jnp.concatenate([pool[a, 2 * g + t, pl.ds(i, 4, stride=2), :] for t in range(2)], axis=0)
                for i in range(2)
            ]
            lines = pl.ds(((a // 8) * 16 + g * 8) * 8 + a % 8, 8, stride=8)
            o1[lines, :] = jnp.where(lane < 64, halves[0], halves[1])
    out_one = pltpu.make_async_copy(o1, one_hbm, out_sem.at[0])
    out_one.start()

    for j in range(8):
        quad = jnp.minimum(pairs[pl.ds(j, 32, stride=16), :], pairs[pl.ds(j + 8, 32, stride=16), :])
        lines = jnp.concatenate([quad] * 4, axis=0).T.reshape(4, 4, 8, LANES)
        lines = jnp.minimum(
            jnp.minimum(lines[:, 0], lines[:, 1]), jnp.minimum(lines[:, 2], lines[:, 3])
        )
        pool[pl.ds(16 + (j // 4) * 4, 4), j % 4] = lines
    for a in range(8):
        quarters = [
            jnp.concatenate([pool[16 + a, g, pl.ds(i, 2, stride=4), :] for g in range(4)], axis=0)
            for i in range(4)
        ]
        low = jnp.where(lane < 32, quarters[0], quarters[1])
        high = jnp.where(lane < 96, quarters[2], quarters[3])
        o2[pl.ds(a, 8, stride=8), :] = jnp.where(lane < 64, low, high)
    out_two = pltpu.make_async_copy(o2, two_hbm, out_sem.at[1])
    out_two.start()
    for out in outs:
        out.wait()
    out_one.wait()
    out_two.wait()


def lines_of(block):
    height, length = block.shape
    return (
        block.reshape(height // 8, 8, length // LANES, LANES)
        .transpose(0, 2, 1, 3)
        .reshape(-1, LANES)
    )


def block_of(lines, height):
    return lines.reshape(height // 8, -1, 8, LANES).transpose(0, 2, 1, 3).reshape(height, -1)


def shards(nz, plane, friction, sources):
    np_ = plane[0] * plane[1]
    width = CHUNKS // np_
    f32 = jnp.float32
    anywhere = pl.BlockSpec(memory_space=pltpu.HBM)
    in_vmem = pl.BlockSpec(memory_space=pltpu.VMEM)
    field = pltpu.VMEM((ROWS, 4, 8, LANES), f32)
    flat = pltpu.VMEM((ROWS * CHUNKS, LANES), f32)
    dma = pltpu.SemaphoreType.DMA

    def message(count, items, *halves):
        return pltpu.VMEM((*count, items, *halves, width, LANES), f32)

    def in_hbm(block):
        return pltpu.with_memory_space_constraint(lines_of(block), pltpu.HBM)

    rounds = []
    for items in (3, 2, 3):
        rounds += [message((np_,), items), message((2, np_), items)]
    for sides, items in (((2,), 2), ((2,), 1), ((), 5)):
        rounds += [message(sides, items, 2), message((nz,), items, 2)]
    lines, most = pl.pallas_call(
        functools.partial(kernel, nz, plane),
        out_shape=(jax.ShapeDtypeStruct((1024, LANES), f32), jax.ShapeDtypeStruct((width, LANES), f32)),
        in_specs=[anywhere, anywhere],
        out_specs=(in_vmem, in_vmem),
        scratch_shapes=[
            flat,
            pltpu.VMEM((ROWS * CHUNKS, LANES), jnp.int32),
            field, field, field, field,
            flat, flat, flat, flat, flat,
            *rounds,
            message((2, 2, np_), 2),
            message((2, np_), 2),
            pltpu.VMEM((width, LANES), f32),
            pltpu.VMEM((np_, width, LANES), f32),
            message((np_,), 4, 2),
            pltpu.VMEM((2, 4, 8, LANES), f32),
            pltpu.VMEM((2, 8, LANES), f32),
            pltpu.VMEM((2, 8, LANES), f32),
            pltpu.VMEM((30, 8, LANES), f32),
            dma((2,)),
            dma((3,)), dma((3, 2)),
            dma((3,)), dma((3,)),
            dma((3, 2)), dma((3,)),
            dma((2,)), dma((2,)),
        ],
        compiler_params=pltpu.CompilerParams(
            collective_id=0, has_side_effects=True, vmem_limit_bytes=16 * 1024 * 1024
        ),
    )(in_hbm(friction), in_hbm(sources))
    cost, one, two, change = pl.pallas_call(
        finish,
        out_shape=(
            jax.ShapeDtypeStruct((1024, LANES), f32),
            jax.ShapeDtypeStruct((256, LANES), f32),
            jax.ShapeDtypeStruct((64, LANES), f32),
            jax.ShapeDtypeStruct((1,), f32),
        ),
        in_specs=[in_vmem, in_vmem],
        out_specs=(anywhere,) * 4,
        scratch_shapes=[
            flat,
            pltpu.VMEM((512, LANES), f32),
            pltpu.VMEM((24, 4, 8, LANES), f32),
            pltpu.VMEM((256, LANES), f32),
            pltpu.VMEM((64, LANES), f32),
            pltpu.SMEM((1,), f32),
            dma((5,)),
        ],
        compiler_params=pltpu.CompilerParams(vmem_limit_bytes=16 * 1024 * 1024),
    )(lines, most)
    return (block_of(cost, 32), block_of(one, 16), block_of(two, 8), change)


def solution(mesh):
    slabs = mesh.shape["rows"]
    plane = PLANE if slabs >= 32 else (2, 2)
    return jax.shard_map(
        functools.partial(shards, slabs // (plane[0] * plane[1]), plane),
        mesh=mesh,
        in_specs=(P("rows", "cols"), P("rows", "cols")),
        out_specs=(P("rows", "cols"), P("rows", "cols"), P("rows", "cols"), P()),
        check_vma=False,
    )
```

```python
import functools

import jax
import jax.numpy as jnp
from jax import lax
from jax.experimental import pallas as pl
from jax.experimental.pallas import tpu as pltpu
from jax.sharding import PartitionSpec as P

HUGE = 1e30
MESH = pl.DeviceIdType.MESH
ROWS = 32
CHUNKS = 32
LANES = 128
PLANE = (4, 4)
HUB = 1
PARTS = 4
STEPS = LANES // PARTS


def far_first(sizes):
    offsets = [()]
    for size in sizes:
        offsets = [(*o, k) for o in offsets for k in range(size)]
    hops = lambda o: sum(min(k, s - k) for k, s in zip(o, sizes))
    return sorted((o for o in offsets if any(o)), key=hops, reverse=True)


def kernel(
    nz, plane, f_hbm, s_hbm, lines_ref, most_ref,
    fn, sn, h_ref, x_ref, d_ref, u_ref, ht, xt, vf, vb, edge,
    s1a, r1a, s1b, r1b, s1c, r1c, s2a, r2a, s2b, r2b, s2c, r2c, s3, r3, s3c, r3c, pre, enter, xs, xr, paths,
    in_sem, send1, recv1, send2, recv2, send3, recv3, sendx, recvx,
):
    px, py = plane
    np_ = px * py
    width = CHUNKS // np_
    row = lax.axis_index("rows")
    core = lax.axis_index("cols")
    z, p = lax.div(row, np_), lax.rem(row, np_)
    x, y = lax.div(p, py), lax.rem(p, py)
    other_core = 1 - core
    hub = core == HUB
    tile = (4, 8, LANES)
    part = (2, width, LANES)
    near_plane = far_first(plane)
    near_z = far_first((nz,))

    loads = (
        pltpu.make_async_copy(f_hbm, fn, in_sem.at[0]),
        pltpu.make_async_copy(s_hbm, sn, in_sem.at[1]),
    )
    for load in loads:
        load.start()

    x_at = [x] + [lax.rem(x + d, px) for d in range(1, px)]
    y_at = [y] + [lax.rem(y + d, py) for d in range(1, py)]
    z_at = [z] + [lax.rem(z + d, nz) for d in range(1, nz)]

    def slot(k):
        dx, dy = near_plane[k]
        return x_at[dx] * py + y_at[dy]

    def z_slot(k):
        return z_at[near_z[k][0]]

    barrier = pltpu.get_barrier_semaphore()

    def greet(device):
        pl.semaphore_signal(barrier, inc=1, device_id=device, device_id_type=MESH)

    @pl.when(hub)
    def _():
        for k in range(np_ - 1):
            greet((z * np_ + slot(k), HUB))
            if k < nz - 1:
                greet((z_slot(k) * np_ + p, HUB))
            greet((z * np_ + slot(k), 1 - HUB))
        greet((row, 1 - HUB))

    def wait_for_peers():
        @pl.when(hub)
        def _():
            pl.semaphore_wait(barrier, np_ - 1 + nz - 1)

        @pl.when(jnp.logical_not(hub))
        def _():
            pl.semaphore_wait(barrier, np_)

    huge = jnp.full(tile, HUGE, jnp.float32)
    zero = jnp.zeros(tile, jnp.float32)

    def spread(b, _):
        for s in range(8):
            for g in range(4):
                lines = pl.ds((b * 32 + g * 8) * 8 + s, 8, stride=8)
                h_ref[b * 8 + s, g] = 0.5 * fn[lines, :]
                x_ref[b * 8 + s, g] = jnp.where(sn[lines, :] == 1, 0.0, HUGE)
        return 0

    for load in loads:
        load.wait()
    lax.fori_loop(0, ROWS // 8, spread, 0)

    def border_costs(b, carry):
        down, up, hd, hu = carry
        for s in range(8):
            i = b * 8 + s
            h = h_ref[i]
            down = jnp.minimum(x_ref[i], down + (hd + h))
            hd = h
            h = h_ref[ROWS - 1 - i]
            up = jnp.minimum(x_ref[ROWS - 1 - i], up + (hu + h))
            hu = h
        return (down, up, hd, hu)

    def add_rows(b, total):
        return sum((h_ref[b * 8 + s] for s in range(8)), start=total)

    def second_local(b, carry):
        down, up, hd, hu, far_d, far_u, most = carry
        for s in range(8):
            i = b * 8 + s
            h, v = h_ref[i], x_ref[i]
            down = jnp.minimum(v, down + (hd + h))
            far_d = jnp.maximum(v, far_d - (hd + h))
            most = jnp.maximum(most, v - down)
            hd = h
            h, v = h_ref[ROWS - 1 - i], x_ref[ROWS - 1 - i]
            up = jnp.minimum(v, up + (hu + h))
            far_u = jnp.maximum(v, far_u - (hu + h))
            most = jnp.maximum(most, v - up)
            hu = h
        return (down, up, hd, hu, far_d, far_u, most)

    def put(to, item, value):
        for q in range(np_):
            line = q * width
            to[q, item] = value[line // 8, line % 8 : line % 8 + width, :]

    def remote(src, dst, send, recv, device):
        return pltpu.make_async_remote_copy(
            src_ref=src, dst_ref=dst, send_sem=send, recv_sem=recv,
            device_id=device, device_id_type=MESH,
        )

    my_z = jnp.full(part, z, jnp.int32)
    last = np_ - 1
    not_hub = jnp.logical_not(hub)

    def to_hub(to, got, n, k):
        q = p if k == last else slot(k)
        return remote(
            to.at[q], got.at[core, p], send1.at[n // 2], recv1.at[n, core], (z * np_ + q, HUB)
        )

    def send_to_hubs(to, got, n):
        for k in range(last):
            to_hub(to, got, n, k).start()

        @pl.when(not_hub)
        def _():
            to_hub(to, got, n, last).start()

    def arrived(ref, sem):
        remote(ref, ref, send1.at[0], sem, (row, HUB)).wait_recv()

    def sent(ref, sem):
        remote(ref, ref, sem, recv1.at[0, 0], (row, HUB)).wait_send()

    def sent_to_hubs(to, got, n):
        @pl.when(hub)
        def _():
            sent(to.at[pl.ds(0, last)], send1.at[n // 2])

        @pl.when(not_hub)
        def _():
            sent(to, send1.at[n // 2])

    def hub_has(to, got, n):
        for item in range(to.shape[1]):
            got[HUB, p, item] = to[p, item]
        arrived(got.at[HUB, pl.ds(0, last)], recv1.at[n, HUB])
        arrived(got.at[1 - HUB], recv1.at[n, 1 - HUB])

    def along_z(source, got, n, k):
        return remote(
            source(k), got.at[z], send2.at[n // 2], recv2.at[n], (z_slot(k) * np_ + p, HUB)
        )

    def by_side(to):
        return lambda k: to.at[lax.div(z_slot(k) - z + nz, nz)]

    def from_hub(source, got, n, half, k):
        q = p if k == last else slot(k)
        return remote(
            source(half, q), got.at[p], send3.at[n // 2, half], recv3.at[n], (z * np_ + q, half)
        )

    to_cores = [(half, k) for k in range(np_) for half in (1 - HUB, HUB) if (half, k) != (HUB, last)]

    def cores_have(got, n):
        @pl.when(hub)
        def _():
            arrived(got.at[pl.ds(0, last)], recv3.at[n])

        @pl.when(not_hub)
        def _():
            arrived(got, recv3.at[n])

    def sent_to_cores(got, n):
        sent(got, send3.at[n // 2, 1 - HUB])
        sent(got.at[pl.ds(0, last)], send3.at[n // 2, HUB])

    def plain(ref):
        return lambda *_: ref

    near = jnp.full(part, HUGE, jnp.float32)
    none = jnp.zeros(part, jnp.float32)
    rounds = ((s1a, r1a, s2a, r2a), (s1b, r1b, s2b, r2b))

    def vertical(step, window):
        s1, r1, s2, r2 = rounds[step]
        down, up, hd, hu = lax.fori_loop(0, ROWS // 8, border_costs, (huge, huge, zero, zero))
        put(s1, 0, up + hu)
        put(s1, 1, down + hd)
        if step == 0:
            put(s1, 2, 2.0 * lax.fori_loop(0, ROWS // 8, add_rows, zero))
            wait_for_peers()
        send_to_hubs(s1, r1, step)
        window()
        to, got = s3.at[step], r3.at[step]

        @pl.when(hub)
        def _():
            hub_has(s1, r1, step)
            b, a, s_down, s_up = near, near, none, none
            for q in range(np_):
                s = r1a[:, q, 2]
                if step == 0:
                    pre[q, 2] = s_down
                    s_down = s_down + s
                pre[q, 0] = b
                b = jnp.minimum(r1[:, q, 1], b + s)
            for q in range(np_ - 1, -1, -1):
                s = r1a[:, q, 2]
                if step == 0:
                    pre[q, 3] = s_up
                    s_up = s_up + s
                pre[q, 1] = a
                a = jnp.minimum(r1[:, q, 0], a + s)
            for side, value in enumerate((a, b)):
                s2[side, 0] = value
                if step == 0:
                    s2[side, 1] = s_down
            for k in range(nz - 1):
                along_z(by_side(s2), r2, step, k).start()
            r2[z, 0] = b
            if step == 0:
                r2[z, 1] = s_down
            else:
                hub_has(s1c, r1c, 2)
                b, far_d, far_u, most = near, -near, -near, none
                for q in range(np_):
                    s, r_p = r1a[:, q, 2], r1c[:, q, 0]
                    most = jnp.maximum(most, jnp.maximum(far_d - r1[:, q, 0], r_p - b))
                    most = jnp.maximum(most, r1c[:, q, 2])
                    far_d = jnp.maximum(r1c[:, q, 1], far_d - s)
                    b = jnp.minimum(r1[:, q, 1], b + s)
                for q in range(np_ - 1, -1, -1):
                    far_u = jnp.maximum(r1c[:, q, 0], far_u - r1a[:, q, 2])
                for item, value in enumerate((a, b, far_u, far_d, most)):
                    s2c[item] = value
                    r2c[z, item] = value
                for k in range(nz - 1):
                    along_z(plain(s2c), r2c, 2, k).start()
            arrived(r2.at[pl.ds(0, nz - 1)], recv2.at[step])
            in_d, in_u = near, near
            for k in range(nz):
                in_d = jnp.where(my_z > k, jnp.minimum(r2[k, 0], in_d + r2a[k, 1]), in_d)
            for k in range(nz - 1, -1, -1):
                in_u = jnp.where(my_z < k, jnp.minimum(r2[k, 0], in_u + r2a[k, 1]), in_u)
            for q in range(np_):
                to[:, q, 0] = jnp.minimum(pre[q, 0], in_d + pre[q, 2])
                to[:, q, 1] = jnp.minimum(pre[q, 1], in_u + pre[q, 3])
            for half, k in to_cores:
                from_hub(lambda h, q: to.at[h, q], got, step, half, k).start()
            for item in range(2):
                got[p, item] = to[HUB, p, item]
            if step == 1:
                arrived(r2c.at[pl.ds(0, nz - 1)], recv2.at[2])
                b, far_d, most = near, -near, none
                for k in range(nz):
                    s = r2a[k, 1]
                    most = jnp.maximum(most, jnp.maximum(far_d - r2c[k, 0], r2c[k, 2] - b))
                    most = jnp.maximum(most, r2c[k, 4])
                    far_d = jnp.maximum(r2c[k, 3], far_d - s)
                    b = jnp.minimum(r2c[k, 1], b + s)
                most = jnp.maximum(most[0], most[1])
                s3c[...] = most
                r3c[p] = most
                for half, k in to_cores:
                    from_hub(plain(s3c), r3c, 2, half, k).start()

        cores_have(got, step)
        for q in range(np_):
            line = q * width
            for item in range(2):
                enter[item, line // 8, line % 8 : line % 8 + width, :] = got[q, item]

        def final(b, carry):
            down, up, hd, hu = carry
            for s in range(8):
                i = b * 8 + s
                h = h_ref[i]
                down = jnp.minimum(x_ref[i], down + (hd + h))
                d_ref[i] = down
                hd = h
                h = h_ref[ROWS - 1 - i]
                up = jnp.minimum(x_ref[ROWS - 1 - i], up + (hu + h))
                u_ref[ROWS - 1 - i] = up
                hu = h
            return (down, up, hd, hu)

        lax.fori_loop(0, ROWS // 8, final, (enter[0], enter[1], zero, zero))

    def second_window():
        _, _, hd, hu, far_d, far_u, most = lax.fori_loop(
            0, ROWS // 8, second_local, (huge, huge, zero, zero, -huge, -huge, zero)
        )
        put(s1c, 0, far_u - hu)
        put(s1c, 1, far_d - hd)
        put(s1c, 2, most)
        send_to_hubs(s1c, r1c, 2)

    def drain(step):
        s1, r1, s2, r2 = rounds[step]
        sent_to_hubs(s1, r1, step)
        to, got = s3.at[step], r3.at[step]
        if step == 1:
            sent_to_hubs(s1c, r1c, 2)
            cores_have(r3c, 2)

        @pl.when(hub)
        def _():
            sent(r2.at[pl.ds(0, nz - 1)], send2.at[0])
            sent_to_cores(got, step)
            if step == 1:
                sent(r2c.at[pl.ds(0, nz - 1)], send2.at[1])
                sent_to_cores(r3c, 2)

    lane = lax.broadcasted_iota(jnp.int32, (8, LANES), 1)
    sub = lax.broadcasted_iota(jnp.int32, (8, LANES), 0)
    inner, outer = lane % 8, sub % 4
    huge2 = jnp.full((8, LANES), HUGE, jnp.float32)
    zero2 = jnp.zeros((8, LANES), jnp.float32)

    def block(load, j):
        return load(pl.ds((j // 4) * 16, 16), j % 4).reshape(LANES, LANES)

    def at(i):
        return pl.ds(pl.multiple_of(i * 8, 8), 8)

    def chunk_path(shift):
        return paths[11 + shift]

    def group_path(shift):
        return paths[22 + shift]

    def measure():
        for j in range(8):
            ht[pl.ds(j, LANES, stride=8), :] = block(lambda r, g: h_ref[r, g], j).T

        def add(b, sums):
            return tuple(
                sum((ht[at(k * STEPS + b * 8 + s), :] for s in range(8)), start=sums[k])
                for k in range(PARTS)
            )

        sums = lax.fori_loop(0, STEPS // 8, add, (zero2,) * PARTS)
        for k in range(PARTS):
            paths[k] = 2.0 * sums[k]
        whole = 2.0 * (sums[0] + sums[1] + sums[2] + sums[3])
        before = after = zero2
        for k in range(-7, 8):
            rolled = pltpu.roll(whole, k % LANES, 1)
            paths[11 + k] = rolled
            if k > 0:
                before = jnp.where(inner >= k, before + rolled, before)
            if k < 0:
                after = jnp.where(inner - k < 8, after + rolled, after)
        paths[26] = before
        paths[27] = after
        whole = before + whole + after
        before = after = zero2
        for k in range(-3, 4):
            rolled = pltpu.roll(whole, k % 8, 0)
            paths[22 + k] = rolled
            if k > 0:
                before = jnp.where(outer >= k, before + rolled, before)
            if k < 0:
                after = jnp.where(outer - k < 4, after + rolled, after)
        paths[28] = before
        paths[29] = after

        def border(b, path):
            for t in range(8):
                i = b * 8 + t
                i = core * i + other_core * (LANES - 1 - i)
                h = ht[at(i), :]
                edge[at(i), :] = path + h
                path = path + 2.0 * h
            return path

        first = jnp.full((8, LANES), core, jnp.int32) == 0
        lax.fori_loop(
            0, LANES // 8, border, jnp.where(first, paths[27] + paths[29], paths[26] + paths[28])
        )

    def scan_all(c, path, axis, size, place, forward):
        step = 1 if forward else -1
        extent = c.shape[axis]
        at_place = place if forward else size - 1 - place
        run = huge2
        for k in range(size - 1, 0, -1):
            ck = pltpu.roll(c, (step * k) % extent, axis)
            run = jnp.where(at_place >= k, jnp.minimum(ck, run + path(step * k)), run)
        before = run
        run = jnp.minimum(c, run + path(0))
        for k in range(1, size):
            ck = pltpu.roll(c, (-step * k) % extent, axis)
            run = jnp.where(at_place + k < size, jnp.minimum(ck, run + path(-step * k)), run)
        return before, run

    def horizontal(step, window):
        for j in range(8):
            rows = pl.ds(j, LANES, stride=8)
            xt[rows, :] = block(lambda r, g: jnp.minimum(d_ref[r, g], u_ref[r, g]), j).T

        def sweep(start_f, start_b, store):
            def some(b, carry):
                right, left, hr, hl = (list(c) for c in carry)
                for s in range(8):
                    for k in range(PARTS):
                        i = k * STEPS + b * 8 + s
                        h = ht[at(i), :]
                        right[k] = jnp.minimum(xt[at(i), :], right[k] + (hr[k] + h))
                        if store:
                            vf[at(i), :] = right[k]
                        hr[k] = h
                        i = (k + 1) * STEPS - 1 - (b * 8 + s)
                        h = ht[at(i), :]
                        left[k] = jnp.minimum(xt[at(i), :], left[k] + (hl[k] + h))
                        if store:
                            vb[at(i), :] = left[k]
                        hl[k] = h
                return (tuple(right), tuple(left), tuple(hr), tuple(hl))

            zeros = (zero2,) * PARTS
            return lax.fori_loop(0, STEPS // 8, some, (start_f, start_b, zeros, zeros))

        right, left, hr, hl = sweep((huge2,) * PARTS, (huge2,) * PARTS, False)
        right = [r + h for r, h in zip(right, hr)]
        left = [r + h for r, h in zip(left, hl)]
        c_f, c_b = right[0], left[-1]
        for k in range(1, PARTS):
            c_f = jnp.minimum(right[k], c_f + paths[k])
            c_b = jnp.minimum(left[-1 - k], c_b + paths[PARTS - 1 - k])
        fc, f_all = scan_all(c_f, chunk_path, 1, 8, inner, True)
        bc, b_all = scan_all(c_b, chunk_path, 1, 8, inner, False)
        gfc, gf_all = scan_all(f_all, group_path, 0, 4, outer, True)
        gbc, gb_all = scan_all(b_all, group_path, 0, 4, outer, False)
        first = jnp.full((8, LANES), core, jnp.int32) == 0
        xs[step] = jnp.where(first, gf_all, gb_all)
        copy = remote(xs.at[step], xr.at[step], sendx.at[0], recvx.at[step], (row, other_core))
        copy.start()
        in_f = [jnp.minimum(fc, gfc + paths[26])]
        in_b = [jnp.minimum(bc, gbc + paths[27])]
        for k in range(PARTS - 1):
            in_f.append(jnp.minimum(right[k], in_f[k] + paths[k]))
            in_b.append(jnp.minimum(left[-1 - k], in_b[k] + paths[PARTS - 1 - k]))
        sweep(tuple(in_f), tuple(in_b[::-1]), True)

        def merge(b, _):
            for t in range(16):
                i = at(b * 16 + t)
                xt[i, :] = jnp.minimum(vf[i, :], vb[i, :])
            return 0

        lax.fori_loop(0, 8, merge, 0)
        window()
        copy.wait()
        return xr[step]

    def in_row(other, j):
        rows = pl.ds(j, LANES, stride=8)
        return jnp.minimum(xt[rows, :], edge[rows, :] + other[j : j + 1])

    vertical(0, measure)
    other = horizontal(0, lambda: drain(0))
    for j in range(8):
        back = in_row(other, j).T
        x_ref[pl.ds((j // 4) * 16, 16), j % 4] = back.reshape(16, 8, LANES)
    vertical(1, second_window)
    other = horizontal(1, lambda: drain(1))
    most = r3c[0]
    for q in range(1, np_):
        most = jnp.maximum(most, r3c[q])
    most_ref[...] = most

    def merge(b, _):
        for t in range(16):
            i = at(b * 16 + t)
            lines_ref[i, :] = jnp.minimum(xt[i, :], edge[i, :] + other)
        return 0

    lax.fori_loop(0, 8, merge, 0)


def finish(xt, most, cost_hbm, one_hbm, two_hbm, change_hbm, on, pairs, pool, o1, o2, change, out_sem):
    lane = lax.broadcasted_iota(jnp.int32, (8, LANES), 1)
    change[0] = jnp.max(most[...])
    outs = [pltpu.make_async_copy(change, change_hbm, out_sem.at[4])]
    outs[0].start()
    for j in range(8):
        back = xt[pl.ds(j, LANES, stride=8), :].T
        for r in range(16):
            i = (j // 4) * 16 + r
            lines = pl.ds(((i // 8) * 32 + (j % 4) * 8) * 8 + i % 8, 8, stride=8)
            on[lines, :] = back[r * 8 : (r + 1) * 8, :]
        if j % 4 == 3:
            half = pl.ds((j // 4) * 512, 512)
            outs.append(pltpu.make_async_copy(on.at[half], cost_hbm.at[half], out_sem.at[2 + j // 4]))
            outs[-1].start()

    for j in range(8):
        pair = jnp.minimum(xt[pl.ds(j, 64, stride=16), :], xt[pl.ds(j + 8, 64, stride=16), :])
        lines = jnp.concatenate([pair, pair], axis=0).T.reshape(8, 2, 8, LANES)
        pool[pl.ds((j // 4) * 8, 8), j % 4] = jnp.minimum(lines[:, 0], lines[:, 1])
        pairs[pl.ds(j, 64, stride=8), :] = pair
    for a in range(16):
        for g in range(2):
            halves = [
                jnp.concatenate([pool[a, 2 * g + t, pl.ds(i, 4, stride=2), :] for t in range(2)], axis=0)
                for i in range(2)
            ]
            lines = pl.ds(((a // 8) * 16 + g * 8) * 8 + a % 8, 8, stride=8)
            o1[lines, :] = jnp.where(lane < 64, halves[0], halves[1])
    out_one = pltpu.make_async_copy(o1, one_hbm, out_sem.at[0])
    out_one.start()

    for j in range(8):
        quad = jnp.minimum(pairs[pl.ds(j, 32, stride=16), :], pairs[pl.ds(j + 8, 32, stride=16), :])
        lines = jnp.concatenate([quad] * 4, axis=0).T.reshape(4, 4, 8, LANES)
        lines = jnp.minimum(
            jnp.minimum(lines[:, 0], lines[:, 1]), jnp.minimum(lines[:, 2], lines[:, 3])
        )
        pool[pl.ds(16 + (j // 4) * 4, 4), j % 4] = lines
    for a in range(8):
        quarters = [
            jnp.concatenate([pool[16 + a, g, pl.ds(i, 2, stride=4), :] for g in range(4)], axis=0)
            for i in range(4)
        ]
        low = jnp.where(lane < 32, quarters[0], quarters[1])
        high = jnp.where(lane < 96, quarters[2], quarters[3])
        o2[pl.ds(a, 8, stride=8), :] = jnp.where(lane < 64, low, high)
    out_two = pltpu.make_async_copy(o2, two_hbm, out_sem.at[1])
    out_two.start()
    for out in outs:
        out.wait()
    out_one.wait()
    out_two.wait()


def lines_of(block):
    height, length = block.shape
    return (
        block.reshape(height // 8, 8, length // LANES, LANES)
        .transpose(0, 2, 1, 3)
        .reshape(-1, LANES)
    )


def block_of(lines, height):
    return lines.reshape(height // 8, -1, 8, LANES).transpose(0, 2, 1, 3).reshape(height, -1)


def shards(nz, plane, friction, sources):
    np_ = plane[0] * plane[1]
    width = CHUNKS // np_
    f32 = jnp.float32
    anywhere = pl.BlockSpec(memory_space=pltpu.HBM)
    in_vmem = pl.BlockSpec(memory_space=pltpu.VMEM)
    field = pltpu.VMEM((ROWS, 4, 8, LANES), f32)
    flat = pltpu.VMEM((ROWS * CHUNKS, LANES), f32)
    dma = pltpu.SemaphoreType.DMA

    def message(count, items, *halves):
        return pltpu.VMEM((*count, items, *halves, width, LANES), f32)

    def in_hbm(block):
        return pltpu.with_memory_space_constraint(lines_of(block), pltpu.HBM)

    rounds = []
    for items in (3, 2, 3):
        rounds += [message((np_,), items), message((2, np_), items)]
    for sides, items in (((2,), 2), ((2,), 1), ((), 5)):
        rounds += [message(sides, items, 2), message((nz,), items, 2)]
    lines, most = pl.pallas_call(
        functools.partial(kernel, nz, plane),
        out_shape=(jax.ShapeDtypeStruct((1024, LANES), f32), jax.ShapeDtypeStruct((width, LANES), f32)),
        in_specs=[anywhere, anywhere],
        out_specs=(in_vmem, in_vmem),
        scratch_shapes=[
            flat,
            pltpu.VMEM((ROWS * CHUNKS, LANES), jnp.int32),
            field, field, field, field,
            flat, flat, flat, flat, flat,
            *rounds,
            message((2, 2, np_), 2),
            message((2, np_), 2),
            pltpu.VMEM((width, LANES), f32),
            pltpu.VMEM((np_, width, LANES), f32),
            message((np_,), 4, 2),
            pltpu.VMEM((2, 4, 8, LANES), f32),
            pltpu.VMEM((2, 8, LANES), f32),
            pltpu.VMEM((2, 8, LANES), f32),
            pltpu.VMEM((30, 8, LANES), f32),
            dma((2,)),
            dma((2,)), dma((3, 2)),
            dma((2,)), dma((3,)),
            dma((2, 2)), dma((3,)),
            dma((1,)), dma((2,)),
        ],
        compiler_params=pltpu.CompilerParams(
            collective_id=0, has_side_effects=True, vmem_limit_bytes=16 * 1024 * 1024
        ),
    )(in_hbm(friction), in_hbm(sources))
    cost, one, two, change = pl.pallas_call(
        finish,
        out_shape=(
            jax.ShapeDtypeStruct((1024, LANES), f32),
            jax.ShapeDtypeStruct((256, LANES), f32),
            jax.ShapeDtypeStruct((64, LANES), f32),
            jax.ShapeDtypeStruct((1,), f32),
        ),
        in_specs=[in_vmem, in_vmem],
        out_specs=(anywhere,) * 4,
        scratch_shapes=[
            flat,
            pltpu.VMEM((512, LANES), f32),
            pltpu.VMEM((24, 4, 8, LANES), f32),
            pltpu.VMEM((256, LANES), f32),
            pltpu.VMEM((64, LANES), f32),
            pltpu.SMEM((1,), f32),
            dma((5,)),
        ],
        compiler_params=pltpu.CompilerParams(vmem_limit_bytes=16 * 1024 * 1024),
    )(lines, most)
    return (block_of(cost, 32), block_of(one, 16), block_of(two, 8), change)


def solution(mesh):
    slabs = mesh.shape["rows"]
    plane = PLANE if slabs >= 32 else (2, 2)
    return jax.shard_map(
        functools.partial(shards, slabs // (plane[0] * plane[1]), plane),
        mesh=mesh,
        in_specs=(P("rows", "cols"), P("rows", "cols")),
        out_specs=(P("rows", "cols"), P("rows", "cols"), P("rows", "cols"), P()),
        check_vma=False,
    )
```
